8 devices in a mesh: dp: 1 (over z), tp: 2 (over y), ep: 4 (over x, core).
Axes of the slice: x: 2, y: 2, z: 1, core: 2. Of those that a mesh axis runs over, the one named last changes fastest.
Arguments:
- hidden: bfloat16 [1024, 768], P(('dp', 'ep'))
- write_pos: int32 [1024], P(('dp', 'ep'))
- enc_mask: int32 [1024, 32], P(('dp', 'ep'))
- expert_idx: int32 [1024], P(('dp', 'ep'))
- self_keys: bfloat16 [2, 1024, 12, 64, 64], P(None, ('dp', 'ep'), 'tp')
- self_values: bfloat16 [2, 1024, 12, 64, 64], P(None, ('dp', 'ep'), 'tp')
- cross_keys: bfloat16 [2, 1024, 12, 32, 64], P(None, ('dp', 'ep'), 'tp')
- cross_values: bfloat16 [2, 1024, 12, 32, 64], P(None, ('dp', 'ep'), 'tp')
- rel_bias: float32 [12, 64], P('tp')
- norm_scale: float32 [2, 3, 768], replicated
- w_query: bfloat16 [2, 768, 768], P(None, None, 'tp')
- w_key: bfloat16 [2, 768, 768], P(None, None, 'tp')
- w_value: bfloat16 [2, 768, 768], P(None, None, 'tp')
- w_out: bfloat16 [2, 768, 768], P(None, 'tp')
- w_cross_query: bfloat16 [2, 768, 768], P(None, None, 'tp')
- w_cross_out: bfloat16 [2, 768, 768], P(None, 'tp')
- dense_gate: bfloat16 [768, 3072], P(None, 'tp')
- dense_up: bfloat16 [768, 3072], P(None, 'tp')
- dense_down: bfloat16 [3072, 768], P('tp')
- router: float32 [768, 32], replicated
- exp_gate: bfloat16 [32, 768, 3072], P('ep', None, 'tp')
- exp_up: bfloat16 [32, 768, 3072], P('ep', None, 'tp')
- exp_down: bfloat16 [32, 3072, 768], P('ep', 'tp')
Outputs:
- output 1: bfloat16 [1024, 768], P(('dp', 'ep'))
- output 2: bfloat16 [2, 1024, 12, 64, 64], P(None, ('dp', 'ep'), 'tp')
- output 3: bfloat16 [2, 1024, 12, 64, 64], P(None, ('dp', 'ep'), 'tp')
All inputs are finite; a program needn't handle non-finite values.
Results may differ from the reference program's by a relative error of at most 0.02.
Values are sent between devices in bfloat16 or wider.
A program may use at most 1 GiB of HBM per device.

```python
import jax
import jax.numpy as jnp
from jax import lax

D = 768
HEADS = 12
HEAD = 64
FF = 3072
EXPERTS = 32
TOK_DEV = 256
GROUPS = 4
CACHE = 64
SRC = 32
TOKENS = TOK_DEV * GROUPS
WIDTH = HEADS * HEAD
CAPACITY = (2 * TOK_DEV + EXPERTS - 1) // EXPERTS
EPS = 1e-6
NEG_BIG = -1e9


def setup_inputs(seed: int = 0, part: int = 0) -> dict:
    root = jax.random.key(seed)
    shared_root, part_root = jax.random.split(root)
    local = jax.random.fold_in(part_root, part)
    local_keys = jax.random.split(local, 10)
    shared_keys = jax.random.split(shared_root, 16)

    def normal(key, shape, scale):
        return jax.random.normal(key, shape, jnp.float32) * scale

    row_ids = jnp.arange(TOKENS)
    hidden = normal(local_keys[0], (TOKENS, D), 1.0).astype(jnp.bfloat16)
    pos_draw = jax.random.randint(local_keys[1], (TOKENS,), 0, CACHE)
    write_pos = jnp.where(row_ids == 0, CACHE - 1, pos_draw).astype(jnp.int32)
    src_len = jax.random.randint(local_keys[2], (TOKENS,), max(SRC // 4, 1), SRC + 1)
    src_len = jnp.where(row_ids == 1, SRC, src_len)
    enc_mask = (jnp.arange(SRC)[None, :] < src_len[:, None]).astype(jnp.int32)
    spread = jax.random.permutation(local_keys[3], TOKENS) % EXPERTS
    hot_expert = jax.random.randint(local_keys[4], (), 0, EXPERTS)
    to_hot = jax.random.randint(local_keys[5], (TOKENS,), 0, 4) == 0
    expert_idx = jnp.where(to_hot, hot_expert, spread).astype(jnp.int32)
    self_shape = (2, TOKENS, HEADS, CACHE, HEAD)
    cross_shape = (2, TOKENS, HEADS, SRC, HEAD)
    return {
        'hidden': hidden,
        'write_pos': write_pos,
        'enc_mask': enc_mask,
        'expert_idx': expert_idx,
        'self_keys': normal(local_keys[6], self_shape, 1.0).astype(jnp.bfloat16),
        'self_values': normal(local_keys[7], self_shape, 1.0).astype(jnp.bfloat16),
        'cross_keys': normal(local_keys[8], cross_shape, 1.0).astype(jnp.bfloat16),
        'cross_values': normal(local_keys[9], cross_shape, 1.0).astype(jnp.bfloat16),
        'rel_bias': normal(shared_keys[0], (HEADS, CACHE), 1.0),
        'norm_scale': jax.random.uniform(shared_keys[1], (2, 3, D), jnp.float32, 0.5, 1.5),
        'w_query': normal(shared_keys[2], (2, D, WIDTH), 2.0 * (D * HEAD) ** -0.5).astype(jnp.bfloat16),
        'w_key': normal(shared_keys[3], (2, D, WIDTH), D ** -0.5).astype(jnp.bfloat16),
        'w_value': normal(shared_keys[4], (2, D, WIDTH), D ** -0.5).astype(jnp.bfloat16),
        'w_out': normal(shared_keys[5], (2, WIDTH, D), WIDTH ** -0.5).astype(jnp.bfloat16),
        'w_cross_query': normal(shared_keys[6], (2, D, WIDTH), 2.0 * (D * HEAD) ** -0.5).astype(jnp.bfloat16),
        'w_cross_out': normal(shared_keys[7], (2, WIDTH, D), WIDTH ** -0.5).astype(jnp.bfloat16),
        'dense_gate': normal(shared_keys[8], (D, FF), D ** -0.5).astype(jnp.bfloat16),
        'dense_up': normal(shared_keys[9], (D, FF), D ** -0.5).astype(jnp.bfloat16),
        'dense_down': normal(shared_keys[10], (FF, D), FF ** -0.5).astype(jnp.bfloat16),
        'router': normal(shared_keys[11], (D, EXPERTS), 2.0 * D ** -0.5),
        'exp_gate': normal(shared_keys[12], (EXPERTS, D, FF), D ** -0.5).astype(jnp.bfloat16),
        'exp_up': normal(shared_keys[13], (EXPERTS, D, FF), D ** -0.5).astype(jnp.bfloat16),
        'exp_down': normal(shared_keys[14], (EXPERTS, FF, D), 0.5 * (EXPERTS / FF) ** 0.5).astype(jnp.bfloat16),
    }


def rms_norm(h_cur, scale):
    h_float = h_cur.astype(jnp.float32)
    inv_rms = lax.rsqrt(jnp.mean(h_float * h_float, axis=-1, keepdims=True) + EPS)
    return (h_float * inv_rms * scale).astype(jnp.bfloat16)


def add_residual(h_cur, delta):
    return (h_cur.astype(jnp.float32) + delta.astype(jnp.float32)).astype(jnp.bfloat16)


def project(normed, weight):
    return jnp.dot(normed, weight, preferred_element_type=jnp.float32)


def self_attention(normed, write_pos, keys, values, w_query, w_key, w_value, w_out, rel_bias):
    tokens = normed.shape[0]
    query = project(normed, w_query).astype(jnp.bfloat16).reshape(tokens, HEADS, HEAD)
    key_new = project(normed, w_key).astype(jnp.bfloat16).reshape(tokens, HEADS, HEAD)
    value_new = project(normed, w_value).astype(jnp.bfloat16).reshape(tokens, HEADS, HEAD)
    distance = write_pos[:, None] - jnp.arange(CACHE)[None, :]
    at_slot = (distance == 0)[:, None, :, None]
    keys = jnp.where(at_slot, key_new[:, :, None, :], keys)
    values = jnp.where(at_slot, value_new[:, :, None, :], values)
    scores = jnp.einsum('thd,thld->thl', query.astype(jnp.float32), keys.astype(jnp.float32))
    bias = jnp.take(rel_bias, jnp.maximum(distance, 0), axis=1)
    scores = jnp.where((distance >= 0)[:, None, :], scores + jnp.swapaxes(bias, 0, 1), NEG_BIG)
    attn_prob = jax.nn.softmax(scores, axis=-1).astype(jnp.bfloat16)
    context = jnp.einsum('thl,thld->thd', attn_prob.astype(jnp.float32), values.astype(jnp.float32)).astype(jnp.bfloat16)
    attn_out = project(context.reshape(tokens, WIDTH), w_out).astype(jnp.bfloat16)
    return attn_out, keys, values


def cross_attention(normed, enc_mask, keys, values, w_query, w_out):
    tokens = normed.shape[0]
    query = project(normed, w_query).astype(jnp.bfloat16).reshape(tokens, HEADS, HEAD)
    scores = jnp.einsum('thd,thsd->ths', query.astype(jnp.float32), keys.astype(jnp.float32))
    scores = jnp.where((enc_mask > 0)[:, None, :], scores, NEG_BIG)
    attn_prob = jax.nn.softmax(scores, axis=-1).astype(jnp.bfloat16)
    context = jnp.einsum('ths,thsd->thd', attn_prob.astype(jnp.float32), values.astype(jnp.float32)).astype(jnp.bfloat16)
    return project(context.reshape(tokens, WIDTH), w_out).astype(jnp.bfloat16)


def gated_ffn(normed, w_gate, w_up, w_down):
    product = (jax.nn.gelu(project(normed, w_gate)) * project(normed, w_up)).astype(jnp.bfloat16)
    return project(product, w_down).astype(jnp.bfloat16)


def switch_ffn(normed, expert_idx, router, exp_gate, exp_up, exp_down):
    logits = jnp.dot(normed.astype(jnp.float32), router)
    route_prob = jax.nn.softmax(logits, axis=-1)
    gate = jnp.take_along_axis(route_prob, expert_idx[:, None], axis=1)[:, 0]
    onehot = (expert_idx[:, None] == jnp.arange(EXPERTS)[None, :]).astype(jnp.int32)
    onehot = onehot.reshape(GROUPS, TOK_DEV, EXPERTS)
    slot = jnp.sum((jnp.cumsum(onehot, axis=1) - onehot) * onehot, axis=2)
    dispatch = (onehot[..., None] * (slot[:, :, None, None] == jnp.arange(CAPACITY))).astype(jnp.float32)
    x_groups = normed.reshape(GROUPS, TOK_DEV, D).astype(jnp.float32)
    buffers = jnp.einsum('gtec,gtd->egcd', dispatch, x_groups).astype(jnp.bfloat16)
    buffers = buffers.reshape(EXPERTS, GROUPS * CAPACITY, D)

    def run_expert(expert):
        rows, w_gate, w_up, w_down = expert
        return gated_ffn(rows, w_gate, w_up, w_down)

    expert_out = lax.map(run_expert, (buffers, exp_gate, exp_up, exp_down))
    expert_out = expert_out.reshape(EXPERTS, GROUPS, CAPACITY, D).astype(jnp.float32)
    combined = jnp.einsum('gtec,egcd->gtd', dispatch, expert_out).reshape(TOKENS, D)
    return gate[:, None] * combined


def attention_block(layer, h_cur, write_pos, enc_mask, self_keys, self_values, cross_keys, cross_values, rel_bias, norm_scale, w_query, w_key, w_value, w_out, w_cross_query, w_cross_out):
    def one_group(group):
        h_grp, pos_grp, mask_grp, keys_grp, values_grp, ckeys_grp, cvalues_grp = group
        normed = rms_norm(h_grp, norm_scale[layer, 0])
        attn_out, keys_grp, values_grp = self_attention(normed, pos_grp, keys_grp, values_grp, w_query[layer], w_key[layer], w_value[layer], w_out[layer], rel_bias)
        h_grp = add_residual(h_grp, attn_out)
        normed = rms_norm(h_grp, norm_scale[layer, 1])
        cross_out = cross_attention(normed, mask_grp, ckeys_grp, cvalues_grp, w_cross_query[layer], w_cross_out[layer])
        return add_residual(h_grp, cross_out), keys_grp, values_grp

    def grouped(array_in):
        return array_in.reshape((GROUPS, TOK_DEV) + array_in.shape[1:])

    h_grp, keys_new, values_new = lax.map(one_group, (grouped(h_cur), grouped(write_pos), grouped(enc_mask), grouped(self_keys[layer]), grouped(self_values[layer]), grouped(cross_keys[layer]), grouped(cross_values[layer])))
    return h_grp.reshape(TOKENS, D), keys_new.reshape(self_keys.shape[1:]), values_new.reshape(self_values.shape[1:])


def reference(hidden, write_pos, enc_mask, expert_idx, self_keys, self_values, cross_keys, cross_values, rel_bias, norm_scale, w_query, w_key, w_value, w_out, w_cross_query, w_cross_out, dense_gate, dense_up, dense_down, router, exp_gate, exp_up, exp_down):
    h_cur, keys_a, values_a = attention_block(0, hidden, write_pos, enc_mask, self_keys, self_values, cross_keys, cross_values, rel_bias, norm_scale, w_query, w_key, w_value, w_out, w_cross_query, w_cross_out)
    normed = rms_norm(h_cur, norm_scale[0, 2])
    h_cur = add_residual(h_cur, gated_ffn(normed, dense_gate, dense_up, dense_down))
    h_cur, keys_b, values_b = attention_block(1, h_cur, write_pos, enc_mask, self_keys, self_values, cross_keys, cross_values, rel_bias, norm_scale, w_query, w_key, w_value, w_out, w_cross_query, w_cross_out)
    normed = rms_norm(h_cur, norm_scale[1, 2])
    h_cur = add_residual(h_cur, switch_ffn(normed, expert_idx, router, exp_gate, exp_up, exp_down))
    return h_cur, jnp.stack([keys_a, keys_b]), jnp.stack([values_a, values_b])
```

```python
import functools

import jax
import jax.numpy as jnp
from jax import lax
from jax.experimental import pallas as pl
from jax.experimental.pallas import tpu as pltpu
from jax.sharding import PartitionSpec as P

EPS = 1e-6
NEG_BIG = -1e9
F32 = jnp.float32
BF16 = jnp.bfloat16
CHUNKS = 2
VMEM_SPEC = pl.BlockSpec(memory_space=pltpu.VMEM)
ANY_SPEC = pl.BlockSpec(memory_space=pl.ANY)
SWAP = [(0, 1), (1, 0)]


def rms_norm(h_cur, scale):
    h_float = h_cur.astype(F32)
    inv_rms = lax.rsqrt(jnp.mean(h_float * h_float, axis=-1, keepdims=True) + EPS)
    return (h_float * inv_rms * scale).astype(BF16)


def project(normed, weight):
    return jnp.dot(normed, weight, preferred_element_type=F32)


def add_parts(h_cur, own, peer):
    total = (own.astype(F32) + peer.astype(F32)).astype(BF16)
    return (h_cur.astype(F32) + total.astype(F32)).astype(BF16)


def softmax_rows(scores):
    top = jnp.max(scores, axis=0, keepdims=True)
    weight = jnp.exp(scores - top)
    return weight / jnp.sum(weight, axis=0, keepdims=True)


def self_kernel(layer, residual, *refs):
    if residual:
        h_ref, own_ref, peer_ref = refs[:3]
        refs = refs[3:]
    else:
        h_ref = refs[0]
        refs = refs[1:]
    pos_ref, scale_ref, bias_ref, wq_ref, wk_ref, wv_ref, wo_ref, k_ref, v_ref = refs[:9]
    refs = refs[9:]
    if len(refs) == 12 + residual:
        refs = refs[2:]
    if residual:
        h_out, refs = refs[0], refs[1:]
    part_ref, ko_ref, vo_ref, q_t, k_t, v_t, ctx_t, prob, posb = refs[:9]
    hot = refs[9]
    head = pl.program_id(0)
    slots, head_dim = k_ref.shape[0], k_ref.shape[1]

    @pl.when(head == 0)
    def _():
        h_cur = h_ref[...]
        if residual:
            h_cur = add_parts(h_cur, own_ref[...], peer_ref[...])
            h_out[...] = h_cur
        x = rms_norm(h_cur, scale_ref[0:1, :])
        q_t[...] = jnp.transpose(project(x, wq_ref[...])).astype(BF16).astype(F32)
        k_t[...] = jnp.transpose(project(x, wk_ref[...])).astype(BF16)
        v_t[...] = jnp.transpose(project(x, wv_ref[...])).astype(BF16)
        pos = pos_ref[...]
        posb[...] = jnp.broadcast_to(pos.astype(F32), posb.shape).astype(BF16)
        rows = lax.broadcasted_iota(jnp.int32, hot.shape, 0)
        hot[...] = (rows == pos).astype(F32)

    rows = pl.ds(pl.multiple_of(head * head_dim, head_dim), head_dim)
    q = q_t[rows, :]
    k_new = k_t[rows, :]
    posv = posb[...]
    for s8 in range(0, slots, 8):
        out_rows = []
        for s in range(s8, s8 + 8):
            cur = jnp.where(posv == jnp.asarray(s, BF16), k_new, k_ref[s])
            ko_ref[s] = cur
            out_rows.append(jnp.sum(cur.astype(F32) * q, axis=0, keepdims=True))
        prob[s8:s8 + 8, :] = jnp.concatenate(out_rows, axis=0)
    line = jnp.broadcast_to(bias_ref[pl.ds(head, 1), :], (slots, 128))
    table = pltpu.roll(line, 0, 1, stride=1, stride_axis=0)
    bias = jnp.dot(table, hot[...], precision=lax.Precision.HIGHEST, preferred_element_type=F32)
    slot_id = lax.broadcasted_iota(jnp.int32, bias.shape, 0)
    scores = jnp.where(slot_id <= pos_ref[...], prob[...] + bias, NEG_BIG)
    prob[...] = softmax_rows(scores).astype(BF16).astype(F32)
    v_new = v_t[rows, :]
    acc = jnp.zeros(q.shape, F32)
    for s in range(slots):
        cur = jnp.where(posv == jnp.asarray(s, BF16), v_new, v_ref[s])
        vo_ref[s] = cur
        acc = acc + prob[s:s + 1, :] * cur.astype(F32)
    ctx_t[rows, :] = acc

    @pl.when(head == pl.num_programs(0) - 1)
    def _():
        ctx = jnp.transpose(ctx_t[...]).astype(BF16)
        part_ref[...] = project(ctx, wo_ref[...]).astype(BF16)


def self_call(layer, chunk, h_cur, parts, pos, scale, bias, wq, wk, wv, wo, keys, values, outs):
    heads, slots, head_dim, tokens = keys.shape[1:]
    tc = tokens // CHUNKS
    dim = wq.shape[1]
    width = wq.shape[2]
    residual = parts is not None

    def whole(rows, cols):
        return pl.BlockSpec((None, rows, cols), lambda i: (layer, 0, 0))

    row_spec = pl.BlockSpec((tc, dim), lambda i: (chunk if h_cur.shape[0] != tc else 0, 0))
    fixed = pl.BlockSpec((tc, dim), lambda i: (0, 0))
    cache = pl.BlockSpec((None, None, slots, head_dim, tc), lambda i: (layer, i, 0, 0, chunk))
    in_specs = [row_spec] + ([fixed, fixed] if residual else [])
    in_specs += [pl.BlockSpec((1, tc), lambda i: (0, chunk)), whole(3, dim), pl.BlockSpec(bias.shape, lambda i: (0, 0)), whole(dim, width), whole(dim, width), whole(dim, width), whole(width, dim), cache, cache]
    args = [h_cur] + (list(parts) if residual else []) + [pos, scale, bias, wq, wk, wv, wo, keys, values]
    out_shape = [jax.ShapeDtypeStruct((tc, dim), BF16)] * (1 + residual)
    out_specs = [fixed] * (1 + residual)
    aliases = {}
    if outs is not None:
        aliases = {len(args): len(out_shape), len(args) + 1: len(out_shape) + 1}
        args += list(outs)
        in_specs += [ANY_SPEC, ANY_SPEC]
    out_shape += [jax.ShapeDtypeStruct(keys.shape, BF16)] * 2
    out_specs += [cache, cache]
    size = heads * slots * head_dim * tc
    return pl.pallas_call(
        functools.partial(self_kernel, layer, residual),
        grid=(heads,),
        in_specs=in_specs,
        out_specs=out_specs,
        out_shape=out_shape,
        input_output_aliases=aliases,
        scratch_shapes=[
            pltpu.VMEM((width, tc), F32),
            pltpu.VMEM((width, tc), BF16),
            pltpu.VMEM((width, tc), BF16),
            pltpu.VMEM((width, tc), F32),
            pltpu.VMEM((slots, tc), F32),
            pltpu.VMEM((head_dim, tc), BF16),
            pltpu.VMEM((128, tc), F32),
        ],
        compiler_params=pltpu.CompilerParams(dimension_semantics=("arbitrary",), vmem_limit_bytes=40 << 20),
        cost_estimate=pl.CostEstimate(flops=size * 400, bytes_accessed=size * 8, transcendentals=0),
        name=f"self{layer}_{chunk}",
    )(*args)


def cross_kernel(h_ref, own_ref, peer_ref, mask_ref, scale_ref, wq_ref, wo_ref, k_ref, v_ref, h_out, part_ref, q_t, ctx_t, prob):
    step = pl.program_id(0)
    per, slots, head_dim, _ = k_ref.shape

    @pl.when(step == 0)
    def _():
        h_cur = add_parts(h_ref[...], own_ref[...], peer_ref[...])
        h_out[...] = h_cur
        x = rms_norm(h_cur, scale_ref[1:2, :])
        q_t[...] = jnp.transpose(project(x, wq_ref[...])).astype(BF16).astype(F32)

    valid = mask_ref[...] > 0
    for j in range(per):
        rows = pl.ds(pl.multiple_of((step * per + j) * head_dim, head_dim), head_dim)
        q = q_t[rows, :]
        for s8 in range(0, slots, 8):
            out_rows = []
            for s in range(s8, s8 + 8):
                out_rows.append(jnp.sum(k_ref[j, s].astype(F32) * q, axis=0, keepdims=True))
            prob[s8:s8 + 8, :] = jnp.concatenate(out_rows, axis=0)
        scores = jnp.where(valid, prob[...], NEG_BIG)
        prob[...] = softmax_rows(scores).astype(BF16).astype(F32)
        acc = jnp.zeros(q.shape, F32)
        for s in range(slots):
            acc = acc + prob[s:s + 1, :] * v_ref[j, s].astype(F32)
        ctx_t[rows, :] = acc

    @pl.when(step == pl.num_programs(0) - 1)
    def _():
        ctx = jnp.transpose(ctx_t[...]).astype(BF16)
        part_ref[...] = project(ctx, wo_ref[...]).astype(BF16)


def cross_call(layer, chunk, h_cur, parts, mask, scale, wq, wo, keys, values, per=2):
    heads, slots, head_dim, tokens = keys.shape[1:]
    tc = tokens // CHUNKS
    dim = wq.shape[1]
    width = wq.shape[2]

    def whole(rows, cols):
        return pl.BlockSpec((None, rows, cols), lambda i: (layer, 0, 0))

    row_spec = pl.BlockSpec((tc, dim), lambda i: (chunk if h_cur.shape[0] != tc else 0, 0))
    fixed = pl.BlockSpec((tc, dim), lambda i: (0, 0))
    cache = pl.BlockSpec((None, per, slots, head_dim, tc), lambda i: (layer, i, 0, 0, chunk))
    size = heads * slots * head_dim * tc
    return pl.pallas_call(
        cross_kernel,
        grid=(heads // per,),
        in_specs=[row_spec, fixed, fixed, pl.BlockSpec((slots, tc), lambda i: (0, chunk)), whole(3, dim), whole(dim, width), whole(width, dim), cache, cache],
        out_specs=[fixed, fixed],
        out_shape=[jax.ShapeDtypeStruct((tc, dim), BF16)] * 2,
        scratch_shapes=[pltpu.VMEM((width, tc), F32), pltpu.VMEM((width, tc), F32), pltpu.VMEM((slots, tc), F32)],
        compiler_params=pltpu.CompilerParams(dimension_semantics=("arbitrary",), vmem_limit_bytes=32 << 20),
        cost_estimate=pl.CostEstimate(flops=size * 400, bytes_accessed=size * 4, transcendentals=0),
        name=f"cross{layer}_{chunk}",
    )(h_cur, *parts, mask, scale, wq, wo, keys, values)


def dense_kernel(h_ref, own_ref, peer_ref, scale_ref, wg_ref, wu_ref, wd_ref, h_out, part_ref, x_scr, acc):
    step = pl.program_id(0)

    @pl.when(step == 0)
    def _():
        h_cur = add_parts(h_ref[...], own_ref[...], peer_ref[...])
        h_out[...] = h_cur
        x_scr[...] = rms_norm(h_cur, scale_ref[2:3, :])
        acc[...] = jnp.zeros_like(acc)

    x = x_scr[...]
    product = (jax.nn.gelu(project(x, wg_ref[...])) * project(x, wu_ref[...])).astype(BF16)
    acc[...] += project(product, wd_ref[...])

    @pl.when(step == pl.num_programs(0) - 1)
    def _():
        part_ref[...] = acc[...].astype(BF16)


def dense_call(chunk, h_cur, parts, scale, wg, wu, wd, tile=512):
    tc, dim = h_cur.shape
    width = wg.shape[1]
    fixed = pl.BlockSpec((tc, dim), lambda i: (0, 0))
    return pl.pallas_call(
        dense_kernel,
        grid=(width // tile,),
        in_specs=[fixed, fixed, fixed, pl.BlockSpec((None, 3, dim), lambda i: (0, 0, 0)), pl.BlockSpec((dim, tile), lambda i: (0, i)), pl.BlockSpec((dim, tile), lambda i: (0, i)), pl.BlockSpec((tile, dim), lambda i: (i, 0))],
        out_specs=[fixed, fixed],
        out_shape=[jax.ShapeDtypeStruct((tc, dim), BF16)] * 2,
        scratch_shapes=[pltpu.VMEM((tc, dim), BF16), pltpu.VMEM((tc, dim), F32)],
        compiler_params=pltpu.CompilerParams(dimension_semantics=("arbitrary",), vmem_limit_bytes=32 << 20),
        cost_estimate=pl.CostEstimate(flops=6 * tc * dim * width, bytes_accessed=6 * dim * width, transcendentals=0),
        name=f"dense_{chunk}",
    )(h_cur, *parts, scale, wg, wu, wd)


def switch_layer(normed, expert_idx, router, exp_gate, exp_up, exp_down):
    tokens = normed.shape[0]
    experts = router.shape[1]
    capacity = (2 * tokens + experts - 1) // experts
    logits = jnp.dot(normed.astype(F32), router, preferred_element_type=F32)
    route_prob = jax.nn.softmax(logits, axis=-1)
    onehot = (expert_idx[:, None] == jnp.arange(experts)[None, :]).astype(jnp.int32)
    gate = jnp.sum(route_prob * onehot, axis=-1)
    slot = jnp.sum((jnp.cumsum(onehot, axis=0) - onehot) * onehot, axis=-1)
    dispatch = (onehot[:, :, None] * (slot[:, None, None] == jnp.arange(capacity)[None, None, :])).astype(BF16)
    buffers = jnp.einsum('tec,td->ecd', dispatch, normed, preferred_element_type=F32).astype(BF16)
    received = lax.all_to_all(buffers, 'ep', 0, 1, tiled=True)
    gate_in = jnp.einsum('ecd,edf->ecf', received, exp_gate, preferred_element_type=F32)
    lin_in = jnp.einsum('ecd,edf->ecf', received, exp_up, preferred_element_type=F32)
    product = (jax.nn.gelu(gate_in) * lin_in).astype(BF16)
    expert_out = jnp.einsum('ecf,efd->ecd', product, exp_down, preferred_element_type=F32).astype(BF16)
    returned = lax.all_to_all(expert_out, 'ep', 1, 0, tiled=True)
    combined = jnp.einsum('tec,ecd->td', dispatch, returned, preferred_element_type=F32).astype(BF16)
    peer = lax.ppermute(combined, 'tp', SWAP)
    return gate[:, None] * (combined.astype(F32) + peer.astype(F32))


def swap(part):
    return part, lax.ppermute(part, 'tp', SWAP)


def decode_body(hidden, write_pos, enc_mask, expert_idx, self_keys, self_values, cross_keys, cross_values, rel_bias, norm_scale, w_query, w_key, w_value, w_out, w_cross_query, w_cross_out, dense_gate, dense_up, dense_down, router, exp_gate, exp_up, exp_down):
    order = (0, 2, 3, 4, 1)
    keys, values = jnp.transpose(self_keys, order), jnp.transpose(self_values, order)
    ckeys, cvalues = jnp.transpose(cross_keys, order), jnp.transpose(cross_values, order)
    pos = write_pos.reshape(1, -1)
    mask = enc_mask.T
    bias = jnp.pad(rel_bias, ((0, 8 - rel_bias.shape[0]), (0, 128 - rel_bias.shape[1])))
    outs = None
    h_cur = [hidden] * CHUNKS
    parts = [None] * CHUNKS
    for layer in range(2):
        for c in range(CHUNKS):
            res = self_call(layer, c, h_cur[c], parts[c], pos, norm_scale, bias, w_query, w_key, w_value, w_out, keys, values, outs)
            if parts[c] is not None:
                h_cur[c] = res[0]
            parts[c] = swap(res[-3])
            outs = res[-2:]
        for c in range(CHUNKS):
            h_cur[c], part = cross_call(layer, c, h_cur[c], parts[c], mask, norm_scale, w_cross_query, w_cross_out, ckeys, cvalues)
            parts[c] = swap(part)
        if layer == 0:
            for c in range(CHUNKS):
                h_cur[c], part = dense_call(c, h_cur[c], parts[c], norm_scale, dense_gate, dense_up, dense_down)
                parts[c] = swap(part)
    h_all = jnp.concatenate([add_parts(h_cur[c], *parts[c]) for c in range(CHUNKS)])
    normed = rms_norm(h_all, norm_scale[1, 2])
    delta = switch_layer(normed, expert_idx, router, exp_gate, exp_up, exp_down)
    h_all = (h_all.astype(F32) + delta).astype(BF16)
    back = (0, 4, 1, 2, 3)
    return h_all, jnp.transpose(outs[0], back), jnp.transpose(outs[1], back)


def solution(mesh):
    batch = ('dp', 'ep')
    row_spec = P(batch, None)
    vec_spec = P(batch)
    cache_spec = P(None, batch, 'tp', None, None)
    col_spec = P(None, None, 'tp')
    out_rows = P(None, 'tp', None)
    in_specs = (row_spec, vec_spec, row_spec, vec_spec, cache_spec, cache_spec, cache_spec, cache_spec, P('tp', None), P(), col_spec, col_spec, col_spec, out_rows, col_spec, out_rows, P(None, 'tp'), P(None, 'tp'), P('tp', None), P(), P('ep', None, 'tp'), P('ep', None, 'tp'), P('ep', 'tp', None))
    out_specs = (row_spec, cache_spec, cache_spec)
    return jax.shard_map(decode_body, mesh=mesh, in_specs=in_specs, out_specs=out_specs, check_vma=False)
```

```python
import functools

import jax
import jax.numpy as jnp
from jax import lax
from jax.experimental import pallas as pl
from jax.experimental.pallas import tpu as pltpu
from jax.sharding import PartitionSpec as P

EPS = 1e-6
NEG_BIG = -1e9
F32 = jnp.float32
BF16 = jnp.bfloat16
CHUNKS = 2
VMEM_SPEC = pl.BlockSpec(memory_space=pltpu.VMEM)
HBM_SPEC = pl.BlockSpec(memory_space=pltpu.HBM)
SWAP = [(0, 1), (1, 0)]


def rms_norm(h_cur, scale):
    h_float = h_cur.astype(F32)
    inv_rms = lax.rsqrt(jnp.mean(h_float * h_float, axis=-1, keepdims=True) + EPS)
    return (h_float * inv_rms * scale).astype(BF16)


def project(normed, weight):
    return jnp.dot(normed, weight, preferred_element_type=F32)


def add_parts(h_cur, own, peer):
    total = (own.astype(F32) + peer.astype(F32)).astype(BF16)
    return (h_cur.astype(F32) + total.astype(F32)).astype(BF16)


def softmax_rows(scores):
    top = jnp.max(scores, axis=0, keepdims=True)
    weight = jnp.exp(scores - top)
    return weight / jnp.sum(weight, axis=0, keepdims=True)


def self_kernel(layer, chunk, residual, aliased, *refs):
    refs = list(refs)
    h_ref = refs.pop(0)
    if residual:
        own_ref, peer_ref = refs.pop(0), refs.pop(0)
    pos_hbm, scale_hbm, bias_hbm, wq_hbm, wk_hbm, wv_hbm, wo_hbm, k_hbm, v_hbm = refs[:9]
    refs = refs[9 + 2 * aliased:]
    if residual:
        h_out = refs.pop(0)
    part_ref, ko_hbm, vo_hbm, h_scr, pos_scr, scale_scr, bias_scr, line_scr, wq_scr, wk_scr, wv_scr, wo_scr, kbuf, vbuf, q_t, k_t, v_t, ctx_t, prob, posb, hot, small_sem, w_sem, k_sem, v_sem, ko_sem, vo_sem = refs
    heads, slots, head_dim, tc = kbuf.shape
    lanes = pl.ds(chunk * tc, tc)

    small = [
        pltpu.make_async_copy(pos_hbm.at[:, lanes], pos_scr, small_sem.at[0]),
        pltpu.make_async_copy(scale_hbm.at[0], scale_scr, small_sem.at[1]),
        pltpu.make_async_copy(bias_hbm, bias_scr, small_sem.at[2]),
    ]
    sliced = h_ref.shape[0] != tc
    if sliced:
        small.append(pltpu.make_async_copy(h_ref.at[lanes, :], h_scr, small_sem.at[3]))
    for copy in small:
        copy.start()
    weights = [pltpu.make_async_copy(hbm.at[layer], scr, w_sem.at[i]) for i, (hbm, scr) in enumerate(((wq_hbm, wq_scr), (wk_hbm, wk_scr), (wv_hbm, wv_scr), (wo_hbm, wo_scr)))]
    for copy in weights[:3]:
        copy.start()

    def fetch_k(head):
        return pltpu.make_async_copy(k_hbm.at[layer, head, :, :, lanes], kbuf.at[head], k_sem.at[head])

    def fetch_v(head):
        return pltpu.make_async_copy(v_hbm.at[layer, head, :, :, lanes], vbuf.at[head], v_sem.at[head])

    def store_k(head):
        return pltpu.make_async_copy(kbuf.at[head], ko_hbm.at[layer, head, :, :, lanes], ko_sem.at[head])

    def store_v(head):
        return pltpu.make_async_copy(vbuf.at[head], vo_hbm.at[layer, head, :, :, lanes], vo_sem.at[head])

    for head in range(heads):
        fetch_k(head).start()
        fetch_v(head).start()
    weights[3].start()
    for copy in small:
        copy.wait()
    if residual:
        h_cur = add_parts(h_ref[...], own_ref[...], peer_ref[...])
        h_out[...] = h_cur
    else:
        h_cur = h_scr[...] if sliced else h_ref[...]
    x = rms_norm(h_cur, scale_scr[layer:layer + 1, :])
    pos = pos_scr[...]
    posb[...] = jnp.broadcast_to(pos.astype(F32), posb.shape).astype(BF16)
    hot[...] = (lax.broadcasted_iota(jnp.int32, hot.shape, 0) == pos).astype(F32)
    line_scr[...] = jnp.zeros_like(line_scr)
    line_scr[0:heads, 0:slots] = bias_scr[...]
    weights[0].wait()
    q_t[...] = jnp.transpose(project(x, wq_scr[...])).astype(BF16).astype(F32)
    weights[1].wait()
    k_t[...] = jnp.transpose(project(x, wk_scr[...])).astype(BF16)
    weights[2].wait()
    v_t[...] = jnp.transpose(project(x, wv_scr[...])).astype(BF16)
    posv = posb[...]

    @pl.loop(0, heads)
    def _(head):
        rows = pl.ds(pl.multiple_of(head * head_dim, head_dim), head_dim)
        q = q_t[rows, :]
        k_new = k_t[rows, :]
        fetch_k(head).wait()
        for s8 in range(0, slots, 8):
            out_rows = []
            for s in range(s8, s8 + 8):
                cur = jnp.where(posv == jnp.asarray(s, BF16), k_new, kbuf[head, s])
                kbuf[head, s] = cur
                out_rows.append(jnp.sum(cur.astype(F32) * q, axis=0, keepdims=True))
            prob[s8:s8 + 8, :] = jnp.concatenate(out_rows, axis=0)
        store_k(head).start()
        line = jnp.broadcast_to(line_scr[pl.ds(head, 1), :], (slots, 128))
        table = pltpu.roll(line, 0, 1, stride=1, stride_axis=0)
        bias = jnp.dot(table, hot[...], precision=lax.Precision.HIGHEST, preferred_element_type=F32)
        slot_id = lax.broadcasted_iota(jnp.int32, bias.shape, 0)
        scores = jnp.where(slot_id <= pos_scr[...], prob[...] + bias, NEG_BIG)
        prob[...] = softmax_rows(scores).astype(BF16).astype(F32)
        v_new = v_t[rows, :]
        fetch_v(head).wait()
        acc = jnp.zeros(q.shape, F32)
        for s in range(slots):
            cur = jnp.where(posv == jnp.asarray(s, BF16), v_new, vbuf[head, s])
            vbuf[head, s] = cur
            acc = acc + prob[s:s + 1, :] * cur.astype(F32)
        store_v(head).start()
        ctx_t[rows, :] = acc

    weights[3].wait()
    ctx = jnp.transpose(ctx_t[...]).astype(BF16)
    part_ref[...] = project(ctx, wo_scr[...]).astype(BF16)
    for head in range(heads):
        store_k(head).wait()
        store_v(head).wait()


def self_call(layer, chunk, h_cur, parts, pos, scale, bias, wq, wk, wv, wo, keys, values, outs):
    heads, slots, head_dim, tokens = keys.shape[1:]
    tc = tokens // CHUNKS
    dim, width = wq.shape[1:]
    residual = parts is not None
    aliased = outs is not None
    in_specs = [VMEM_SPEC] * 3 if residual else [VMEM_SPEC if h_cur.shape[0] == tc else HBM_SPEC]
    in_specs += [HBM_SPEC] * 9
    args = [h_cur] + (list(parts) if residual else []) + [pos, scale, bias, wq, wk, wv, wo, keys, values]
    rows = jax.ShapeDtypeStruct((tc, dim), BF16)
    out_shape = [rows] * (1 + residual) + [jax.ShapeDtypeStruct(keys.shape, BF16)] * 2
    out_specs = [VMEM_SPEC] * (1 + residual) + [HBM_SPEC] * 2
    aliases = {}
    if aliased:
        aliases = {len(args): 1 + residual, len(args) + 1: 2 + residual}
        args += list(outs)
        in_specs += [HBM_SPEC] * 2
    size = heads * slots * head_dim * tc
    return pl.pallas_call(
        functools.partial(self_kernel, layer, chunk, residual, aliased),
        in_specs=in_specs,
        out_specs=out_specs,
        out_shape=out_shape,
        input_output_aliases=aliases,
        scratch_shapes=[
            pltpu.VMEM((tc, dim), BF16),
            pltpu.VMEM((1, tc), jnp.int32),
            pltpu.VMEM(scale.shape[1:], F32),
            pltpu.VMEM(bias.shape, F32),
            pltpu.VMEM((8, 128), F32),
            pltpu.VMEM((dim, width), BF16),
            pltpu.VMEM((dim, width), BF16),
            pltpu.VMEM((dim, width), BF16),
            pltpu.VMEM((width, dim), BF16),
            pltpu.VMEM((heads, slots, head_dim, tc), BF16),
            pltpu.VMEM((heads, slots, head_dim, tc), BF16),
            pltpu.VMEM((width, tc), F32),
            pltpu.VMEM((width, tc), BF16),
            pltpu.VMEM((width, tc), BF16),
            pltpu.VMEM((width, tc), F32),
            pltpu.VMEM((slots, tc), F32),
            pltpu.VMEM((head_dim, tc), BF16),
            pltpu.VMEM((128, tc), F32),
            pltpu.SemaphoreType.DMA((4,)),
            pltpu.SemaphoreType.DMA((4,)),
            pltpu.SemaphoreType.DMA((heads,)),
            pltpu.SemaphoreType.DMA((heads,)),
            pltpu.SemaphoreType.DMA((heads,)),
            pltpu.SemaphoreType.DMA((heads,)),
        ],
        compiler_params=pltpu.CompilerParams(vmem_limit_bytes=48 << 20),
        cost_estimate=pl.CostEstimate(flops=size * 400, bytes_accessed=size * 8, transcendentals=0),
        name=f"self{layer}_{chunk}",
    )(*args)


def tp_peer():
    return (lax.axis_index('dp'), 1 - lax.axis_index('tp'), lax.axis_index('ep'))


def remote(src, dst, sems, device):
    return pltpu.make_async_remote_copy(src_ref=src, dst_ref=dst, send_sem=sems[0], recv_sem=sems[1], device_id=device, device_id_type=pl.DeviceIdType.MESH)


def greet(devices):
    barrier = pltpu.get_barrier_semaphore()
    for device in devices:
        pl.semaphore_signal(barrier, inc=1, device_id=device, device_id_type=pl.DeviceIdType.MESH)
    pl.semaphore_wait(barrier, len(devices))


def cross_part(x, keys, values, mask_t, wq, wo, q_t, ctx_t, prob, before_attention, out_ref):
    heads, slots, head_dim, _ = keys.shape
    q_t[...] = jnp.transpose(project(x, wq[...])).astype(BF16).astype(F32)
    before_attention()

    @pl.loop(0, heads)
    def _(head):
        rows = pl.ds(pl.multiple_of(head * head_dim, head_dim), head_dim)
        q = q_t[rows, :]
        for s8 in range(0, slots, 8):
            out_rows = []
            for s in range(s8, s8 + 8):
                out_rows.append(jnp.sum(keys[head, s].astype(F32) * q, axis=0, keepdims=True))
            prob[s8:s8 + 8, :] = jnp.concatenate(out_rows, axis=0)
        scores = jnp.where(mask_t > 0, prob[...], NEG_BIG)
        prob[...] = softmax_rows(scores).astype(BF16).astype(F32)
        acc = jnp.zeros(q.shape, F32)
        for s in range(slots):
            acc = acc + prob[s:s + 1, :] * values[head, s].astype(F32)
        ctx_t[rows, :] = acc

    ctx = jnp.transpose(ctx_t[...]).astype(BF16)
    out_ref[...] = project(ctx, wo[...]).astype(BF16)


def cross_scratch(heads, slots, head_dim, tokens, dim):
    tc = tokens // 2
    width = heads * head_dim
    return dict(
        scale_scr=pltpu.VMEM((3, 2, dim), F32),
        mask_scr=pltpu.VMEM((slots, tokens), jnp.int32),
        wq_scr=pltpu.VMEM((dim, width), BF16),
        wo_scr=pltpu.VMEM((width, dim), BF16),
        kbuf=pltpu.VMEM((2, heads, slots, head_dim, tc), BF16),
        vbuf=pltpu.VMEM((2, heads, slots, head_dim, tc), BF16),
        q_t=pltpu.VMEM((width, tc), F32),
        ctx_t=pltpu.VMEM((width, tc), F32),
        prob=pltpu.VMEM((slots, tc), F32),
        sbuf=pltpu.VMEM((3, tc, dim), BF16),
        rbuf=pltpu.VMEM((4, tc, dim), BF16),
        send_sem=pltpu.SemaphoreType.DMA((4,)),
        recv_sem=pltpu.SemaphoreType.DMA((4,)),
        c_sem=pltpu.SemaphoreType.DMA((8,)),
    )


class Cross:
    def __init__(self, layer, r, t, count):
        self.layer, self.r, self.t = layer, r, t
        tc = t.sbuf.shape[1]
        self.loads = [
            pltpu.make_async_copy(r.scale, t.scale_scr, t.c_sem.at[0]),
            pltpu.make_async_copy(r.mask, t.mask_scr, t.c_sem.at[1]),
            pltpu.make_async_copy(r.wq.at[layer], t.wq_scr, t.c_sem.at[2]),
            pltpu.make_async_copy(r.wo.at[layer], t.wo_scr, t.c_sem.at[3]),
        ]
        self.kv = []
        for c in range(2):
            lanes = pl.ds(c * tc, tc)
            self.kv.append([
                pltpu.make_async_copy(r.keys.at[layer, :, :, :, lanes], t.kbuf.at[c], t.c_sem.at[4 + 2 * c]),
                pltpu.make_async_copy(r.values.at[layer, :, :, :, lanes], t.vbuf.at[c], t.c_sem.at[5 + 2 * c]),
            ])
        peer = tp_peer()
        sources = [r.p_b] + [t.sbuf.at[i] for i in range(3)]
        self.swaps = [remote(sources[i], t.rbuf.at[i], (t.send_sem.at[i], t.recv_sem.at[i]), peer) for i in range(count)]
        self.tc = tc

    def start_loads(self):
        for copy in self.loads + self.kv[0] + self.kv[1]:
            copy.start()

    def run(self):
        t, r = self.t, self.r
        self.swaps[0].start()
        for copy in self.loads:
            copy.wait()
        streams = []
        for c in range(2):
            if c == 0:
                h_cur = add_parts(r.h_a[...], r.p_a[...], r.peer_a[...])
            else:
                self.swaps[0].wait_recv()
                h_cur = add_parts(r.h_b[...], r.p_b[...], t.rbuf[0])
            streams.append(h_cur)
            x = rms_norm(h_cur, t.scale_scr[1, self.layer:self.layer + 1, :])

            def ready():
                for copy in self.kv[c]:
                    copy.wait()

            cross_part(x, t.kbuf.at[c], t.vbuf.at[c], t.mask_scr[:, c * self.tc:(c + 1) * self.tc], t.wq_scr, t.wo_scr, t.q_t, t.ctx_t, t.prob, ready, t.sbuf.at[c])
            self.swaps[1 + c].start()
        return streams


class Refs:
    def __init__(self, names, refs):
        self.__dict__.update(zip(names, refs, strict=True))


CROSS_IN = ('h_a', 'h_b', 'p_a', 'peer_a', 'p_b', 'mask', 'scale', 'wq', 'wo', 'keys', 'values')


def dense_part(x, wg, wu, wd, acc, out_ref, tile=512):
    acc[...] = jnp.zeros_like(acc)

    @pl.loop(0, wg.shape[1] // tile)
    def _(i):
        cols = pl.ds(pl.multiple_of(i * tile, tile), tile)
        product = (jax.nn.gelu(project(x, wg[:, cols])) * project(x, wu[:, cols])).astype(BF16)
        acc[...] += project(product, wd[cols, :])

    out_ref[...] = acc[...].astype(BF16)


def block_a_kernel(names, *refs):
    r = t = Refs(names, refs)
    cross = Cross(0, r, t, 4)
    cross.start_loads()
    dense = [pltpu.make_async_copy(src, dst, t.d_sem.at[i]) for i, (src, dst) in enumerate(((r.wg, t.wg_scr), (r.wu, t.wu_scr), (r.wd, t.wd_scr)))]
    for copy in dense:
        copy.start()
    greet([tp_peer()])
    h_a, h_b = cross.run()
    r.h2_a[...] = h_a
    r.h2_b[...] = h_b
    for copy in dense:
        copy.wait()
    scale = t.scale_scr[2, 0:1, :]
    cross.swaps[1].wait_recv()
    h_a = add_parts(r.h2_a[...], t.sbuf[0], t.rbuf[1])
    r.h2_a[...] = h_a
    dense_part(rms_norm(h_a, scale), t.wg_scr, t.wu_scr, t.wd_scr, t.acc, t.sbuf.at[2])
    cross.swaps[3].start()
    cross.swaps[2].wait_recv()
    h_b = add_parts(r.h2_b[...], t.sbuf[1], t.rbuf[2])
    r.h2_b[...] = h_b
    dense_part(rms_norm(h_b, scale), t.wg_scr, t.wu_scr, t.wd_scr, t.acc, r.pd_b)
    cross.swaps[3].wait_recv()
    r.h2_a[...] = add_parts(r.h2_a[...], t.sbuf[2], t.rbuf[3])
    for copy in cross.swaps:
        copy.wait_send()


def block_a_call(h_a, h_b, p_a, peer_a, p_b, mask, scale, wq, wo, keys, values, wg, wu, wd):
    _, heads, slots, head_dim, tokens = keys.shape
    dim, ff = wg.shape
    tc = tokens // 2
    scratch = cross_scratch(heads, slots, head_dim, tokens, dim)
    scratch.update(
        wg_scr=pltpu.VMEM((dim, ff), BF16),
        wu_scr=pltpu.VMEM((dim, ff), BF16),
        wd_scr=pltpu.VMEM((ff, dim), BF16),
        acc=pltpu.VMEM((tc, dim), F32),
        d_sem=pltpu.SemaphoreType.DMA((3,)),
    )
    names = CROSS_IN + ('wg', 'wu', 'wd', 'h2_a', 'h2_b', 'pd_b') + tuple(scratch)
    rows = jax.ShapeDtypeStruct((tc, dim), BF16)
    return pl.pallas_call(
        functools.partial(block_a_kernel, names),
        in_specs=[VMEM_SPEC] * 5 + [HBM_SPEC] * 9,
        out_specs=[VMEM_SPEC] * 3,
        out_shape=[rows] * 3,
        scratch_shapes=list(scratch.values()),
        compiler_params=pltpu.CompilerParams(vmem_limit_bytes=56 << 20, collective_id=0, has_side_effects=True),
        cost_estimate=pl.CostEstimate(flops=20_000_000_000, bytes_accessed=20 << 20, transcendentals=0),
        name="block_a",
    )(h_a, h_b, p_a, peer_a, p_b, mask, scale, wq, wo, keys, values, wg, wu, wd)


def block_b_kernel(names, *refs):
    r = t = Refs(names, refs)
    dp, tp, me = lax.axis_index('dp'), lax.axis_index('tp'), lax.axis_index('ep')
    group = lax.axis_size('ep')
    local, cap_rows, dim = t.xin.shape
    capacity = cap_rows // group
    tokens = t.x_scr.shape[0]
    ring = t.wg_ring.shape[0]
    tc = tokens // 2
    others = [(dp, tp, lax.rem(me + k, group)) for k in range(1, group)]

    def fetch(i):
        slot = lax.rem(i, ring)
        return [pltpu.make_async_copy(src.at[i], dst.at[slot], t.e_sem.at[n, slot]) for n, (src, dst) in enumerate(((r.wg, t.wg_ring), (r.wu, t.wu_ring), (r.wd, t.wd_ring)))]

    cross = Cross(1, r, t, 3)
    cross.start_loads()
    side = [pltpu.make_async_copy(r.router, t.router_scr, t.s_sem.at[0]), pltpu.make_async_copy(r.idx, t.idx_scr, t.s_sem.at[1])]
    for copy in side:
        copy.start()
    for i in range(ring):
        for copy in fetch(i):
            copy.start()
    greet([tp_peer()] + others)
    h_a, h_b = cross.run()
    t.h_scr[0:tc, :] = h_a
    t.h_scr[tc:, :] = h_b

    for copy in side:
        copy.wait()
    lane_idx = jnp.broadcast_to(t.idx_scr[...].astype(F32), (tokens, tokens))
    row_idx = jnp.transpose(lane_idx)
    same = lane_idx == row_idx
    row_no = lax.broadcasted_iota(jnp.int32, same.shape, 0)
    lane_no = lax.broadcasted_iota(jnp.int32, same.shape, 1)
    lane_slot = jnp.sum(jnp.where(same & (row_no < lane_no), 1.0, 0.0), axis=0, keepdims=True)
    row_slot = jnp.sum(jnp.where(same & (lane_no < row_no), 1.0, 0.0), axis=1, keepdims=True)
    total = group * local * capacity
    lane_dest = jnp.where(lane_slot < capacity, lane_idx[0:1, :] * capacity + lane_slot, -1.0)
    row_dest = jnp.where(row_slot < capacity, row_idx[:, 0:1] * capacity + row_slot, -1.0)
    t.pick[...] = (lax.broadcasted_iota(jnp.int32, (total, tokens), 0).astype(F32) == lane_dest).astype(BF16)
    t.place[...] = (lax.broadcasted_iota(jnp.int32, (tokens, total), 1).astype(F32) == row_dest).astype(BF16)
    expert_hot = lax.broadcasted_iota(jnp.int32, (tokens, group * local), 1).astype(F32) == row_idx[:, 0:1]

    for c in range(2):
        rows = slice(c * tc, (c + 1) * tc)
        cross.swaps[1 + c].wait_recv()
        h_cur = add_parts(t.h_scr[rows, :], t.sbuf[c], t.rbuf[1 + c])
        t.h_scr[rows, :] = h_cur
        t.x_scr[rows, :] = rms_norm(h_cur, t.scale_scr[2, 1:2, :])
    t.disp[...] = project(t.pick[...], t.x_scr[...]).astype(BF16)

    def span(owner, i):
        return pl.ds(pl.multiple_of((owner * local + i) * capacity, capacity), capacity)

    def mine(owner):
        return pl.ds(pl.multiple_of(owner * capacity, capacity), capacity)

    def send_rows(i, k):
        dst = lax.rem(me + k, group)
        return remote(t.disp.at[span(dst, i), :], t.xin.at[i, mine(me), :], (t.ds_sem.at[k - 1, i], t.dr_sem.at[k - 1, i]), (dp, tp, dst))

    def send_back(i, k):
        dst = lax.rem(me + k, group)
        return remote(t.yout.at[i, mine(dst), :], t.ret.at[span(me, i), :], (t.bs_sem.at[k - 1, i], t.br_sem.at[k - 1, i]), (dp, tp, dst))

    @pl.loop(0, local)
    def _(i):
        for k in range(1, group):
            send_rows(i, k).start()
        t.xin[i, mine(me), :] = t.disp[span(me, i), :]

    logits = jnp.dot(t.x_scr[...].astype(F32), t.router_scr[...].T, precision=lax.Precision.HIGHEST, preferred_element_type=F32)
    top = jnp.max(logits, axis=-1, keepdims=True)
    weight = jnp.exp(logits - top)
    weight = weight / jnp.sum(weight, axis=-1, keepdims=True)
    t.gate[...] = jnp.broadcast_to(jnp.sum(jnp.where(expert_hot, weight, 0.0), axis=-1, keepdims=True), t.gate.shape)

    @pl.loop(0, local)
    def _(i):
        slot = lax.rem(i, ring)
        for k in range(1, group):
            send_rows(i, k).wait_recv()
        copies = fetch(i)
        x = t.xin[i]
        copies[0].wait()
        gate_in = jax.nn.gelu(project(x, t.wg_ring[slot]))
        copies[1].wait()
        product = (gate_in * project(x, t.wu_ring[slot])).astype(BF16)
        copies[2].wait()
        t.yout[i] = project(product, t.wd_ring[slot]).astype(BF16)
        for k in range(1, group):
            send_back(i, k).start()
        t.ret[span(me, i), :] = t.yout[i, mine(me), :]

        @pl.when(i + ring < local)
        def _():
            for copy in fetch(i + ring):
                copy.start()

    @pl.loop(0, local)
    def _(i):
        for k in range(1, group):
            send_back(i, k).wait_recv()

    pieces = t.comb.shape[0]
    size = tokens // pieces
    last = [remote(t.comb.at[p], t.comb_peer.at[p], (t.fs_sem.at[p], t.fr_sem.at[p]), tp_peer()) for p in range(pieces)]
    for p in range(pieces):
        t.comb[p] = project(t.place[p * size:(p + 1) * size, :], t.ret[...]).astype(BF16)
        last[p].start()
    for p in range(pieces):
        rows = slice(p * size, (p + 1) * size)
        last[p].wait_recv()
        both = (t.comb[p].astype(F32) + t.comb_peer[p].astype(F32))
        gate = t.gate[rows, 0:1]
        r.out[rows, :] = (t.h_scr[rows, :].astype(F32) + gate * both).astype(BF16)
    for copy in cross.swaps + last:
        copy.wait_send()

    @pl.loop(0, local)
    def _(i):
        for k in range(1, group):
            send_rows(i, k).wait_send()
            send_back(i, k).wait_send()


def block_b_call(h_a, h_b, p_a, peer_a, p_b, mask, scale, wq, wo, keys, values, router, idx, wg, wu, wd, group):
    _, heads, slots, head_dim, tokens = keys.shape
    local, dim, ff = wg.shape
    experts = router.shape[0]
    capacity = (2 * tokens + experts - 1) // experts
    ring = 5
    pieces = 4
    scratch = cross_scratch(heads, slots, head_dim, tokens, dim)
    hops = (group - 1, local)
    scratch.update(
        wg_ring=pltpu.VMEM((ring, dim, ff), BF16),
        wu_ring=pltpu.VMEM((ring, dim, ff), BF16),
        wd_ring=pltpu.VMEM((ring, ff, dim), BF16),
        router_scr=pltpu.VMEM(router.shape, F32),
        idx_scr=pltpu.VMEM((1, tokens), jnp.int32),
        h_scr=pltpu.VMEM((tokens, dim), BF16),
        x_scr=pltpu.VMEM((tokens, dim), BF16),
        pick=pltpu.VMEM((experts * capacity, tokens), BF16),
        place=pltpu.VMEM((tokens, experts * capacity), BF16),
        gate=pltpu.VMEM((tokens, 128), F32),
        disp=pltpu.VMEM((experts * capacity, dim), BF16),
        xin=pltpu.VMEM((local, group * capacity, dim), BF16),
        yout=pltpu.VMEM((local, group * capacity, dim), BF16),
        ret=pltpu.VMEM((experts * capacity, dim), BF16),
        comb=pltpu.VMEM((pieces, tokens // pieces, dim), BF16),
        comb_peer=pltpu.VMEM((pieces, tokens // pieces, dim), BF16),
        e_sem=pltpu.SemaphoreType.DMA((3, ring)),
        s_sem=pltpu.SemaphoreType.DMA((2,)),
        ds_sem=pltpu.SemaphoreType.DMA(hops),
        dr_sem=pltpu.SemaphoreType.DMA(hops),
        bs_sem=pltpu.SemaphoreType.DMA(hops),
        br_sem=pltpu.SemaphoreType.DMA(hops),
        fs_sem=pltpu.SemaphoreType.DMA((pieces,)),
        fr_sem=pltpu.SemaphoreType.DMA((pieces,)),
    )
    names = CROSS_IN + ('router', 'idx', 'wg', 'wu', 'wd', 'out') + tuple(scratch)
    return pl.pallas_call(
        functools.partial(block_b_kernel, names),
        in_specs=[VMEM_SPEC] * 5 + [HBM_SPEC] * 11,
        out_specs=VMEM_SPEC,
        out_shape=jax.ShapeDtypeStruct((tokens, dim), BF16),
        scratch_shapes=list(scratch.values()),
        compiler_params=pltpu.CompilerParams(vmem_limit_bytes=63 << 20, collective_id=1, has_side_effects=True),
        cost_estimate=pl.CostEstimate(flops=40_000_000_000, bytes_accessed=70 << 20, transcendentals=0),
        name="block_b",
    )(h_a, h_b, p_a, peer_a, p_b, mask, scale, wq, wo, keys, values, router, idx, wg, wu, wd)


def swap(part):
    return part, lax.ppermute(part, 'tp', SWAP)


def decode_body(hidden, write_pos, enc_mask, expert_idx, self_keys, self_values, cross_keys, cross_values, rel_bias, norm_scale, w_query, w_key, w_value, w_out, w_cross_query, w_cross_out, dense_gate, dense_up, dense_down, router, exp_gate, exp_up, exp_down):
    order = (0, 2, 3, 4, 1)
    keys, values = jnp.transpose(self_keys, order), jnp.transpose(self_values, order)
    ckeys, cvalues = jnp.transpose(cross_keys, order), jnp.transpose(cross_values, order)
    pos = write_pos.reshape(1, -1)
    mask = enc_mask.T
    scale = jnp.transpose(norm_scale, (1, 0, 2))
    shared = (pos, scale, rel_bias, w_query, w_key, w_value, w_out, keys, values)
    cross = (mask, scale, w_cross_query, w_cross_out, ckeys, cvalues)
    p_a, *outs = self_call(0, 0, hidden, None, *shared, None)
    pair_a = swap(p_a)
    p_b, *outs = self_call(0, 1, hidden, None, *shared, outs)
    h_a, h_b = hidden[:hidden.shape[0] // 2], hidden[hidden.shape[0] // 2:]
    h_a, h_b, pd_b = block_a_call(h_a, h_b, *pair_a, p_b, *cross, dense_gate, dense_up, dense_down)
    pair_b = swap(pd_b)
    p_a, *outs = self_call(1, 0, h_a, None, *shared, outs)
    pair_a = swap(p_a)
    h_b, p_b, *outs = self_call(1, 1, h_b, pair_b, *shared, outs)
    h_all = block_b_call(h_a, h_b, *pair_a, p_b, *cross, router.T, expert_idx.reshape(1, -1), exp_gate, exp_up, exp_down, lax.axis_size('ep'))
    back = (0, 4, 1, 2, 3)
    return h_all, jnp.transpose(outs[0], back), jnp.transpose(outs[1], back)


def solution(mesh):
    batch = ('dp', 'ep')
    row_spec = P(batch, None)
    vec_spec = P(batch)
    cache_spec = P(None, batch, 'tp', None, None)
    col_spec = P(None, None, 'tp')
    out_rows = P(None, 'tp', None)
    in_specs = (row_spec, vec_spec, row_spec, vec_spec, cache_spec, cache_spec, cache_spec, cache_spec, P('tp', None), P(), col_spec, col_spec, col_spec, out_rows, col_spec, out_rows, P(None, 'tp'), P(None, 'tp'), P('tp', None), P(), P('ep', None, 'tp'), P('ep', None, 'tp'), P('ep', 'tp', None))
    out_specs = (row_spec, cache_spec, cache_spec)
    return jax.shard_map(decode_body, mesh=mesh, in_specs=in_specs, out_specs=out_specs, check_vma=False)
```

```python
import functools

import jax
import jax.numpy as jnp
from jax import lax
from jax.experimental import pallas as pl
from jax.experimental.pallas import tpu as pltpu
from jax.sharding import PartitionSpec as P

EPS = 1e-6
NEG_BIG = -1e9
F32 = jnp.float32
BF16 = jnp.bfloat16
CHUNKS = 2
VMEM_SPEC = pl.BlockSpec(memory_space=pltpu.VMEM)
HBM_SPEC = pl.BlockSpec(memory_space=pltpu.HBM)
SWAP = [(0, 1), (1, 0)]


def rms_norm(h_cur, scale):
    h_float = h_cur.astype(F32)
    inv_rms = lax.rsqrt(jnp.mean(h_float * h_float, axis=-1, keepdims=True) + EPS)
    return (h_float * inv_rms * scale).astype(BF16)


def project(normed, weight):
    return jnp.dot(normed, weight, preferred_element_type=F32)


def add_parts(h_cur, own, peer):
    total = (own.astype(F32) + peer.astype(F32)).astype(BF16)
    return (h_cur.astype(F32) + total.astype(F32)).astype(BF16)


def softmax_rows(scores):
    top = jnp.max(scores, axis=0, keepdims=True)
    weight = jnp.exp(scores - top)
    return weight / jnp.sum(weight, axis=0, keepdims=True)


def self_kernel(layer, chunk, residual, aliased, *refs):
    refs = list(refs)
    h_ref = refs.pop(0)
    if residual:
        own_ref, peer_ref = refs.pop(0), refs.pop(0)
    pos_hbm, scale_hbm, bias_hbm, wq_hbm, wk_hbm, wv_hbm, wo_hbm, k_hbm, v_hbm = refs[:9]
    refs = refs[9 + 2 * aliased:]
    if residual:
        h_out = refs.pop(0)
    part_ref, ko_hbm, vo_hbm, h_scr, pos_scr, scale_scr, bias_scr, line_scr, wq_scr, wk_scr, wv_scr, wo_scr, kbuf, vbuf, q_t, k_t, v_t, ctx_t, prob, posb, hot, small_sem, w_sem, k_sem, v_sem, ko_sem, vo_sem = refs
    heads, slots, head_dim, tc = kbuf.shape
    lanes = pl.ds(chunk * tc, tc)

    small = [
        pltpu.make_async_copy(pos_hbm.at[:, lanes], pos_scr, small_sem.at[0]),
        pltpu.make_async_copy(scale_hbm.at[0], scale_scr, small_sem.at[1]),
        pltpu.make_async_copy(bias_hbm, bias_scr, small_sem.at[2]),
    ]
    sliced = h_ref.shape[0] != tc
    if sliced:
        small.append(pltpu.make_async_copy(h_ref.at[lanes, :], h_scr, small_sem.at[3]))
    for copy in small:
        copy.start()
    weights = [pltpu.make_async_copy(hbm.at[layer], scr, w_sem.at[i]) for i, (hbm, scr) in enumerate(((wq_hbm, wq_scr), (wk_hbm, wk_scr), (wv_hbm, wv_scr), (wo_hbm, wo_scr)))]
    for copy in weights[:3]:
        copy.start()

    def fetch_k(head):
        return pltpu.make_async_copy(k_hbm.at[layer, head, :, :, lanes], kbuf.at[head], k_sem.at[head])

    def fetch_v(head):
        return pltpu.make_async_copy(v_hbm.at[layer, head, :, :, lanes], vbuf.at[head], v_sem.at[head])

    def store_k(head):
        return pltpu.make_async_copy(kbuf.at[head], ko_hbm.at[layer, head, :, :, lanes], ko_sem.at[head])

    def store_v(head):
        return pltpu.make_async_copy(vbuf.at[head], vo_hbm.at[layer, head, :, :, lanes], vo_sem.at[head])

    fetch_k(0).start()
    fetch_v(0).start()
    for copy in small:
        copy.wait()
    if residual:
        h_cur = add_parts(h_ref[...], own_ref[...], peer_ref[...])
        h_out[...] = h_cur
    else:
        h_cur = h_scr[...] if sliced else h_ref[...]
    x = rms_norm(h_cur, scale_scr[layer:layer + 1, :])
    pos = pos_scr[...]
    posb[...] = jnp.broadcast_to(pos.astype(F32), posb.shape).astype(BF16)
    hot[...] = (lax.broadcasted_iota(jnp.int32, hot.shape, 0) == pos).astype(F32)
    line_scr[...] = jnp.zeros_like(line_scr)
    line_scr[0:heads, 0:slots] = bias_scr[...]
    for copy in weights[:3]:
        copy.wait()
    for head in range(1, heads):
        fetch_k(head).start()
        fetch_v(head).start()
    weights[3].start()
    q_t[...] = jnp.transpose(project(x, wq_scr[...])).astype(BF16).astype(F32)
    k_t[...] = jnp.transpose(project(x, wk_scr[...])).astype(BF16)
    v_t[...] = jnp.transpose(project(x, wv_scr[...])).astype(BF16)
    posv = posb[...]

    @pl.loop(0, heads)
    def _(head):
        rows = pl.ds(pl.multiple_of(head * head_dim, head_dim), head_dim)
        q = q_t[rows, :]
        k_new = k_t[rows, :]
        fetch_k(head).wait()
        for s8 in range(0, slots, 8):
            out_rows = []
            for s in range(s8, s8 + 8):
                cur = jnp.where(posv == jnp.asarray(s, BF16), k_new, kbuf[head, s])
                kbuf[head, s] = cur
                out_rows.append(jnp.sum(cur.astype(F32) * q, axis=0, keepdims=True))
            prob[s8:s8 + 8, :] = jnp.concatenate(out_rows, axis=0)
        store_k(head).start()
        line = jnp.broadcast_to(line_scr[pl.ds(head, 1), :], (slots, 128))
        table = pltpu.roll(line, 0, 1, stride=1, stride_axis=0)
        bias = jnp.dot(table, hot[...], precision=lax.Precision.HIGHEST, preferred_element_type=F32)
        slot_id = lax.broadcasted_iota(jnp.int32, bias.shape, 0)
        scores = jnp.where(slot_id <= pos_scr[...], prob[...] + bias, NEG_BIG)
        prob[...] = softmax_rows(scores).astype(BF16).astype(F32)
        v_new = v_t[rows, :]
        fetch_v(head).wait()
        acc = jnp.zeros(q.shape, F32)
        for s in range(slots):
            cur = jnp.where(posv == jnp.asarray(s, BF16), v_new, vbuf[head, s])
            vbuf[head, s] = cur
            acc = acc + prob[s:s + 1, :] * cur.astype(F32)
        store_v(head).start()
        ctx_t[rows, :] = acc

    weights[3].wait()
    ctx = jnp.transpose(ctx_t[...]).astype(BF16)
    part_ref[...] = project(ctx, wo_scr[...]).astype(BF16)
    for head in range(heads):
        store_k(head).wait()
        store_v(head).wait()


def self_call(layer, chunk, h_cur, parts, pos, scale, bias, wq, wk, wv, wo, keys, values, outs):
    heads, slots, head_dim, tokens = keys.shape[1:]
    tc = tokens // CHUNKS
    dim, width = wq.shape[1:]
    residual = parts is not None
    aliased = outs is not None
    in_specs = [VMEM_SPEC] * 3 if residual else [VMEM_SPEC if h_cur.shape[0] == tc else HBM_SPEC]
    in_specs += [HBM_SPEC] * 9
    args = [h_cur] + (list(parts) if residual else []) + [pos, scale, bias, wq, wk, wv, wo, keys, values]
    rows = jax.ShapeDtypeStruct((tc, dim), BF16)
    out_shape = [rows] * (1 + residual) + [jax.ShapeDtypeStruct(keys.shape, BF16)] * 2
    out_specs = [VMEM_SPEC] * (1 + residual) + [HBM_SPEC] * 2
    aliases = {}
    if aliased:
        aliases = {len(args): 1 + residual, len(args) + 1: 2 + residual}
        args += list(outs)
        in_specs += [HBM_SPEC] * 2
    size = heads * slots * head_dim * tc
    return pl.pallas_call(
        functools.partial(self_kernel, layer, chunk, residual, aliased),
        in_specs=in_specs,
        out_specs=out_specs,
        out_shape=out_shape,
        input_output_aliases=aliases,
        scratch_shapes=[
            pltpu.VMEM((tc, dim), BF16),
            pltpu.VMEM((1, tc), jnp.int32),
            pltpu.VMEM(scale.shape[1:], F32),
            pltpu.VMEM(bias.shape, F32),
            pltpu.VMEM((8, 128), F32),
            pltpu.VMEM((dim, width), BF16),
            pltpu.VMEM((dim, width), BF16),
            pltpu.VMEM((dim, width), BF16),
            pltpu.VMEM((width, dim), BF16),
            pltpu.VMEM((heads, slots, head_dim, tc), BF16),
            pltpu.VMEM((heads, slots, head_dim, tc), BF16),
            pltpu.VMEM((width, tc), F32),
            pltpu.VMEM((width, tc), BF16),
            pltpu.VMEM((width, tc), BF16),
            pltpu.VMEM((width, tc), F32),
            pltpu.VMEM((slots, tc), F32),
            pltpu.VMEM((head_dim, tc), BF16),
            pltpu.VMEM((128, tc), F32),
            pltpu.SemaphoreType.DMA((4,)),
            pltpu.SemaphoreType.DMA((4,)),
            pltpu.SemaphoreType.DMA((heads,)),
            pltpu.SemaphoreType.DMA((heads,)),
            pltpu.SemaphoreType.DMA((heads,)),
            pltpu.SemaphoreType.DMA((heads,)),
        ],
        compiler_params=pltpu.CompilerParams(vmem_limit_bytes=48 << 20),
        cost_estimate=pl.CostEstimate(flops=size * 400, bytes_accessed=size * 8, transcendentals=0),
        name=f"self{layer}_{chunk}",
    )(*args)


def tp_peer():
    return (lax.axis_index('dp'), 1 - lax.axis_index('tp'), lax.axis_index('ep'))


def remote(src, dst, sems, device):
    return pltpu.make_async_remote_copy(src_ref=src, dst_ref=dst, send_sem=sems[0], recv_sem=sems[1], device_id=device, device_id_type=pl.DeviceIdType.MESH)


def greet(devices):
    barrier = pltpu.get_barrier_semaphore()
    for device in devices:
        pl.semaphore_signal(barrier, inc=1, device_id=device, device_id_type=pl.DeviceIdType.MESH)
    pl.semaphore_wait(barrier, len(devices))


def cross_part(x, keys, values, mask_t, wq, wo, q_t, ctx_t, prob, before_attention, out_ref):
    heads, slots, head_dim, _ = keys.shape
    q_t[...] = jnp.transpose(project(x, wq[...])).astype(BF16).astype(F32)
    before_attention()

    @pl.loop(0, heads)
    def _(head):
        rows = pl.ds(pl.multiple_of(head * head_dim, head_dim), head_dim)
        q = q_t[rows, :]
        for s8 in range(0, slots, 8):
            out_rows = []
            for s in range(s8, s8 + 8):
                out_rows.append(jnp.sum(keys[head, s].astype(F32) * q, axis=0, keepdims=True))
            prob[s8:s8 + 8, :] = jnp.concatenate(out_rows, axis=0)
        scores = jnp.where(mask_t > 0, prob[...], NEG_BIG)
        prob[...] = softmax_rows(scores).astype(BF16).astype(F32)
        acc = jnp.zeros(q.shape, F32)
        for s in range(slots):
            acc = acc + prob[s:s + 1, :] * values[head, s].astype(F32)
        ctx_t[rows, :] = acc

    ctx = jnp.transpose(ctx_t[...]).astype(BF16)
    out_ref[...] = project(ctx, wo[...]).astype(BF16)


def cross_scratch(heads, slots, head_dim, tokens, dim):
    tc = tokens // 2
    width = heads * head_dim
    return dict(
        scale_scr=pltpu.VMEM((3, 2, dim), F32),
        mask_scr=pltpu.VMEM((slots, tokens), jnp.int32),
        wq_scr=pltpu.VMEM((dim, width), BF16),
        wo_scr=pltpu.VMEM((width, dim), BF16),
        kbuf=pltpu.VMEM((2, heads, slots, head_dim, tc), BF16),
        vbuf=pltpu.VMEM((2, heads, slots, head_dim, tc), BF16),
        q_t=pltpu.VMEM((width, tc), F32),
        ctx_t=pltpu.VMEM((width, tc), F32),
        prob=pltpu.VMEM((slots, tc), F32),
        sbuf=pltpu.VMEM((3, tc, dim), BF16),
        rbuf=pltpu.VMEM((4, tc, dim), BF16),
        send_sem=pltpu.SemaphoreType.DMA((4,)),
        recv_sem=pltpu.SemaphoreType.DMA((4,)),
        c_sem=pltpu.SemaphoreType.DMA((8,)),
    )


class Cross:
    def __init__(self, layer, r, t, count):
        self.layer, self.r, self.t = layer, r, t
        tc = t.sbuf.shape[1]
        self.loads = [
            pltpu.make_async_copy(r.scale, t.scale_scr, t.c_sem.at[0]),
            pltpu.make_async_copy(r.mask, t.mask_scr, t.c_sem.at[1]),
            pltpu.make_async_copy(r.wq.at[layer], t.wq_scr, t.c_sem.at[2]),
            pltpu.make_async_copy(r.wo.at[layer], t.wo_scr, t.c_sem.at[3]),
        ]
        self.kv = []
        for c in range(2):
            lanes = pl.ds(c * tc, tc)
            self.kv.append([
                pltpu.make_async_copy(r.keys.at[layer, :, :, :, lanes], t.kbuf.at[c], t.c_sem.at[4 + 2 * c]),
                pltpu.make_async_copy(r.values.at[layer, :, :, :, lanes], t.vbuf.at[c], t.c_sem.at[5 + 2 * c]),
            ])
        peer = tp_peer()
        sources = [r.p_b] + [t.sbuf.at[i] for i in range(3)]
        self.swaps = [remote(sources[i], t.rbuf.at[i], (t.send_sem.at[i], t.recv_sem.at[i]), peer) for i in range(count)]
        self.tc = tc

    def start_loads(self):
        for copy in self.loads[:4] + self.kv[0]:
            copy.start()

    def run(self, later):
        t, r = self.t, self.r
        self.swaps[0].start()
        for copy in self.loads:
            copy.wait()
        for copy in self.kv[1]:
            copy.start()
        streams = []
        for c in range(2):
            if c == 0:
                h_cur = add_parts(r.h_a[...], r.p_a[...], r.peer_a[...])
            else:
                self.swaps[0].wait_recv()
                h_cur = add_parts(r.h_b[...], r.p_b[...], t.rbuf[0])
            streams.append(h_cur)
            x = rms_norm(h_cur, t.scale_scr[1, self.layer:self.layer + 1, :])

            def ready():
                for copy in self.kv[c]:
                    copy.wait()
                if c == 0:
                    for copy in later:
                        copy.start()

            cross_part(x, t.kbuf.at[c], t.vbuf.at[c], t.mask_scr[:, c * self.tc:(c + 1) * self.tc], t.wq_scr, t.wo_scr, t.q_t, t.ctx_t, t.prob, ready, t.sbuf.at[c])
            self.swaps[1 + c].start()
        return streams


class Refs:
    def __init__(self, names, refs):
        self.__dict__.update(zip(names, refs, strict=True))


CROSS_IN = ('h_a', 'h_b', 'p_a', 'peer_a', 'p_b', 'mask', 'scale', 'wq', 'wo', 'keys', 'values')


def dense_part(x, wg, wu, wd, acc, out_ref, tile=512):
    acc[...] = jnp.zeros_like(acc)

    @pl.loop(0, wg.shape[1] // tile)
    def _(i):
        cols = pl.ds(pl.multiple_of(i * tile, tile), tile)
        product = (jax.nn.gelu(project(x, wg[:, cols])) * project(x, wu[:, cols])).astype(BF16)
        acc[...] += project(product, wd[cols, :])

    out_ref[...] = acc[...].astype(BF16)


def block_a_kernel(names, *refs):
    r = t = Refs(names, refs)
    stream = pltpu.make_async_copy(r.hidden, t.h_scr, t.d_sem.at[3])
    stream.start()
    tc = t.acc.shape[0]
    r.h_a, r.h_b = t.h_scr.at[0:tc, :], t.h_scr.at[tc:, :]
    cross = Cross(0, r, t, 4)
    cross.loads.append(stream)
    cross.start_loads()
    dense = [pltpu.make_async_copy(src, dst, t.d_sem.at[i]) for i, (src, dst) in enumerate(((r.wg, t.wg_scr), (r.wu, t.wu_scr), (r.wd, t.wd_scr)))]
    greet([tp_peer()])
    h_a, h_b = cross.run(dense)
    r.h2_a[...] = h_a
    r.h2_b[...] = h_b
    for copy in dense:
        copy.wait()
    scale = t.scale_scr[2, 0:1, :]
    cross.swaps[1].wait_recv()
    h_a = add_parts(r.h2_a[...], t.sbuf[0], t.rbuf[1])
    r.h2_a[...] = h_a
    dense_part(rms_norm(h_a, scale), t.wg_scr, t.wu_scr, t.wd_scr, t.acc, t.sbuf.at[2])
    cross.swaps[3].start()
    cross.swaps[2].wait_recv()
    h_b = add_parts(r.h2_b[...], t.sbuf[1], t.rbuf[2])
    r.h2_b[...] = h_b
    dense_part(rms_norm(h_b, scale), t.wg_scr, t.wu_scr, t.wd_scr, t.acc, r.pd_b)
    cross.swaps[3].wait_recv()
    r.h2_a[...] = add_parts(r.h2_a[...], t.sbuf[2], t.rbuf[3])
    for copy in cross.swaps:
        copy.wait_send()


def block_a_call(hidden, p_a, peer_a, p_b, mask, scale, wq, wo, keys, values, wg, wu, wd):
    _, heads, slots, head_dim, tokens = keys.shape
    dim, ff = wg.shape
    tc = tokens // 2
    scratch = cross_scratch(heads, slots, head_dim, tokens, dim)
    scratch.update(
        wg_scr=pltpu.VMEM((dim, ff), BF16),
        wu_scr=pltpu.VMEM((dim, ff), BF16),
        wd_scr=pltpu.VMEM((ff, dim), BF16),
        acc=pltpu.VMEM((tc, dim), F32),
        h_scr=pltpu.VMEM((tokens, dim), BF16),
        d_sem=pltpu.SemaphoreType.DMA((4,)),
    )
    names = ('hidden',) + CROSS_IN[2:] + ('wg', 'wu', 'wd', 'h2_a', 'h2_b', 'pd_b') + tuple(scratch)
    rows = jax.ShapeDtypeStruct((tc, dim), BF16)
    return pl.pallas_call(
        functools.partial(block_a_kernel, names),
        in_specs=[HBM_SPEC] + [VMEM_SPEC] * 3 + [HBM_SPEC] * 9,
        out_specs=[VMEM_SPEC] * 3,
        out_shape=[rows] * 3,
        scratch_shapes=list(scratch.values()),
        compiler_params=pltpu.CompilerParams(vmem_limit_bytes=48 << 20, collective_id=0, has_side_effects=True),
        cost_estimate=pl.CostEstimate(flops=20_000_000_000, bytes_accessed=20 << 20, transcendentals=0),
        name="block_a",
    )(hidden, p_a, peer_a, p_b, mask, scale, wq, wo, keys, values, wg, wu, wd)


def block_b_kernel(names, *refs):
    r = t = Refs(names, refs)
    dp, tp, me = lax.axis_index('dp'), lax.axis_index('tp'), lax.axis_index('ep')
    group = lax.axis_size('ep')
    local, cap_rows, dim = t.xin.shape
    capacity = cap_rows // group
    tokens = t.h_scr.shape[0]
    ring = t.wg_ring.shape[0]
    tc = tokens // 2
    half = dim // 2
    lag = 3
    rows_local = local * capacity
    near = (dp, tp, me + 1 - 2 * lax.rem(me, 2))
    across = (dp, tp, lax.rem(me + 2, group))
    others = [(dp, tp, lax.rem(me + k, group)) for k in range(1, group)]
    owners = (me, near[2], across[2], lax.rem(near[2] + 2, group))

    def fetch(i):
        slot = lax.rem(i, ring)
        return [pltpu.make_async_copy(src.at[i], dst.at[slot], t.e_sem.at[n, slot]) for n, (src, dst) in enumerate(((r.wg, t.wg_ring), (r.wu, t.wu_ring), (r.wd, t.wd_ring)))]

    cross = Cross(1, r, t, 3)
    cross.start_loads()
    side = [pltpu.make_async_copy(r.router, t.router_scr, t.s_sem.at[0]), pltpu.make_async_copy(r.idx, t.idx_scr, t.s_sem.at[1])]
    for copy in side:
        copy.start()
    greet([tp_peer()] + others)
    early = []
    for i in range(ring):
        early += fetch(i)

    h_a, h_b = cross.run(early)
    t.h_scr[0:tc, :] = h_a
    t.h_scr[tc:, :] = h_b
    def spread(c):
        rows = pl.ds(c * tc, tc)
        mine = t.x_scr.at[0, rows, :]
        return [
            remote(mine, t.x_scr.at[2, rows, :], (t.xs_sem.at[c, 0], t.xr_sem.at[c, 0]), across),
            remote(mine, t.x_scr.at[1, rows, :], (t.xs_sem.at[c, 1], t.xr_sem.at[c, 1]), near),
            remote(t.x_scr.at[2, rows, :], t.x_scr.at[3, rows, :], (t.xs_sem.at[c, 2], t.xr_sem.at[c, 2]), near),
        ]

    def span(owner, i):
        return pl.ds(pl.multiple_of((owner * local + i) * capacity, capacity), capacity)

    def mine(owner):
        return pl.ds(pl.multiple_of(owner * capacity, capacity), capacity)

    def send_back(i, k):
        dst = lax.rem(me + k, group)
        return remote(t.ysum.at[i, mine(dst), :], t.ret.at[span(me, i), :], (t.bs_sem.at[k - 1, i], t.br_sem.at[k - 1, i]), (dp, tp, dst))

    def fold(i):
        return remote(t.yout.at[i], t.yin.at[i], (t.os_sem.at[i], t.or_sem.at[i]), tp_peer())

    def give_back(i):
        fold(i).wait_recv()
        t.ysum[i] = (t.ysum[i].astype(F32) + t.yin[i].astype(F32)).astype(BF16)
        for k in range(1, group):
            send_back(i, k).start()
        t.ret[span(me, i), :] = t.ysum[i, mine(me), :]

    def finish(c):
        rows = slice(c * tc, (c + 1) * tc)
        cross.swaps[1 + c].wait_recv()
        h_cur = add_parts(t.h_scr[rows, :], t.sbuf[c], t.rbuf[1 + c])
        t.h_scr[rows, :] = h_cur
        t.x_scr[0, rows, :] = rms_norm(h_cur, t.scale_scr[2, 1:2, :])
        hops = spread(c)
        hops[0].start()
        hops[1].start()
        return hops

    first = finish(0)
    side[1].wait()
    lane_idx = jnp.broadcast_to(t.idx_scr[...].astype(F32), (tokens, tokens))
    row_idx = jnp.transpose(lane_idx)
    same = lane_idx == row_idx
    row_no = lax.broadcasted_iota(jnp.int32, same.shape, 0)
    lane_no = lax.broadcasted_iota(jnp.int32, same.shape, 1)
    lane_slot = jnp.sum(jnp.where(same & (row_no < lane_no), 1.0, 0.0), axis=0, keepdims=True)
    row_slot = jnp.sum(jnp.where(same & (lane_no < row_no), 1.0, 0.0), axis=1, keepdims=True)
    total = group * rows_local
    lane_dest = jnp.where(lane_slot < capacity, lane_idx[0:1, :] * capacity + lane_slot, -1.0)
    row_dest = jnp.where(row_slot < capacity, row_idx[:, 0:1] * capacity + row_slot, -1.0)
    t.dest[0] = jnp.broadcast_to(lane_dest, t.dest.shape[1:])
    dest_sends = [remote(t.dest.at[0], t.dest.at[k], (t.is_sem.at[k - 1], t.ir_sem.at[k - 1]), (dp, tp, owners[k])) for k in range(1, group)]
    for copy in dest_sends:
        copy.start()
    t.place[...] = (lax.broadcasted_iota(jnp.int32, (tokens, total), 1).astype(F32) == row_dest).astype(BF16)
    t.hot[...] = jnp.where(lax.broadcasted_iota(jnp.int32, t.hot.shape, 1).astype(F32) == row_idx[:, 0:1], 1.0, 0.0)

    second = finish(1)
    first[0].wait_recv()
    first[2].start()
    first_row = (me * rows_local).astype(F32)
    for k in range(group):
        if k:
            dest_sends[k - 1].wait_recv()
        wanted = lax.broadcasted_iota(jnp.int32, (rows_local, tokens), 0).astype(F32) + first_row
        t.pick[k] = (wanted == t.dest[k, 0:1, :]).astype(BF16)
    side[0].wait()
    logits = jnp.dot(t.x_scr[0].astype(F32), t.router_scr[...].T, precision=lax.Precision.HIGHEST, preferred_element_type=F32)
    top = jnp.max(logits, axis=-1, keepdims=True)
    weight = jnp.exp(logits - top)
    weight = weight / jnp.sum(weight, axis=-1, keepdims=True)
    t.gate[...] = jnp.broadcast_to(jnp.sum(t.hot[...] * weight, axis=-1, keepdims=True), t.gate.shape)
    second[0].wait_recv()
    second[2].start()
    for copy in first[1:] + second[1:]:
        copy.wait_recv()
    for k in range(group):
        block = project(t.pick[k], t.x_scr[k]).astype(BF16)
        for i in range(local):
            t.xin[i, mine(owners[k]), :] = block[i * capacity:(i + 1) * capacity, :]

    @pl.loop(0, local)
    def _(i):
        slot = lax.rem(i, ring)
        copies = fetch(i)
        x = t.xin[i]
        copies[0].wait()
        gate_in = jax.nn.gelu(project(x, t.wg_ring[slot]))
        copies[1].wait()
        product = (gate_in * project(x, t.wu_ring[slot])).astype(BF16)
        copies[2].wait()
        result = project(product, t.wd_ring[slot]).astype(BF16)
        low, high = result[:, :half], result[:, half:]
        t.ysum[i] = jnp.where(tp == 0, low, high)
        t.yout[i] = jnp.where(tp == 0, high, low)
        fold(i).start()

        @pl.when(i >= lag)
        def _():
            give_back(i - lag)

        @pl.when(i + ring < local)
        def _():
            for copy in fetch(i + ring):
                copy.start()

    @pl.loop(local - lag, local)
    def _(i):
        give_back(i)

    @pl.loop(0, local)
    def _(i):
        for k in range(1, group):
            send_back(i, k).wait_recv()

    pieces = t.comb.shape[0]
    size = tokens // pieces
    last = [remote(t.comb.at[p], t.comb_peer.at[p], (t.fs_sem.at[p], t.fr_sem.at[p]), tp_peer()) for p in range(pieces)]
    for p in range(pieces):
        t.comb[p] = project(t.place[p * size:(p + 1) * size, :], t.ret[...]).astype(BF16)
        last[p].start()
    for p in range(pieces):
        rows = slice(p * size, (p + 1) * size)
        last[p].wait_recv()
        own, peer = t.comb[p].astype(F32), t.comb_peer[p].astype(F32)
        gate = t.gate[rows, 0:1]
        for side_no, both in enumerate((jnp.where(tp == 0, own, peer), jnp.where(tp == 0, peer, own))):
            cols = slice(side_no * half, (side_no + 1) * half)
            r.out[rows, cols] = (t.h_scr[rows, cols].astype(F32) + gate * both).astype(BF16)
    for copy in cross.swaps + last + dest_sends + first + second:
        copy.wait_send()

    @pl.loop(0, local)
    def _(i):
        fold(i).wait_send()
        for k in range(1, group):
            send_back(i, k).wait_send()


def block_b_call(h_a, h_b, p_a, peer_a, p_b, mask, scale, wq, wo, keys, values, router, idx, wg, wu, wd, group):
    _, heads, slots, head_dim, tokens = keys.shape
    local, dim, ff = wg.shape
    experts = router.shape[0]
    capacity = (2 * tokens + experts - 1) // experts
    ring = 5
    pieces = 4
    scratch = cross_scratch(heads, slots, head_dim, tokens, dim)
    hops = (group - 1, local)
    scratch.update(
        wg_ring=pltpu.VMEM((ring, dim, ff), BF16),
        wu_ring=pltpu.VMEM((ring, dim, ff), BF16),
        wd_ring=pltpu.VMEM((ring, ff, dim), BF16),
        router_scr=pltpu.VMEM(router.shape, F32),
        idx_scr=pltpu.VMEM((1, tokens), jnp.int32),
        h_scr=pltpu.VMEM((tokens, dim), BF16),
        x_scr=pltpu.VMEM((group, tokens, dim), BF16),
        dest=pltpu.VMEM((group, 8, tokens), F32),
        hot=pltpu.VMEM((tokens, experts), F32),
        pick=pltpu.VMEM((group, local * capacity, tokens), BF16),
        place=pltpu.VMEM((tokens, experts * capacity), BF16),
        gate=pltpu.VMEM((tokens, 128), F32),
        xin=pltpu.VMEM((local, group * capacity, dim), BF16),
        yout=pltpu.VMEM((local, group * capacity, dim // 2), BF16),
        yin=pltpu.VMEM((local, group * capacity, dim // 2), BF16),
        ysum=pltpu.VMEM((local, group * capacity, dim // 2), BF16),
        ret=pltpu.VMEM((experts * capacity, dim // 2), BF16),
        comb=pltpu.VMEM((pieces, tokens // pieces, dim // 2), BF16),
        comb_peer=pltpu.VMEM((pieces, tokens // pieces, dim // 2), BF16),
        e_sem=pltpu.SemaphoreType.DMA((3, ring)),
        s_sem=pltpu.SemaphoreType.DMA((2,)),
        is_sem=pltpu.SemaphoreType.DMA((group - 1,)),
        ir_sem=pltpu.SemaphoreType.DMA((group - 1,)),
        xs_sem=pltpu.SemaphoreType.DMA((2, 3)),
        xr_sem=pltpu.SemaphoreType.DMA((2, 3)),
        bs_sem=pltpu.SemaphoreType.DMA(hops),
        br_sem=pltpu.SemaphoreType.DMA(hops),
        os_sem=pltpu.SemaphoreType.DMA((local,)),
        or_sem=pltpu.SemaphoreType.DMA((local,)),
        fs_sem=pltpu.SemaphoreType.DMA((pieces,)),
        fr_sem=pltpu.SemaphoreType.DMA((pieces,)),
    )
    names = CROSS_IN + ('router', 'idx', 'wg', 'wu', 'wd', 'out') + tuple(scratch)
    return pl.pallas_call(
        functools.partial(block_b_kernel, names),
        in_specs=[VMEM_SPEC] * 5 + [HBM_SPEC] * 11,
        out_specs=VMEM_SPEC,
        out_shape=jax.ShapeDtypeStruct((tokens, dim), BF16),
        scratch_shapes=list(scratch.values()),
        compiler_params=pltpu.CompilerParams(vmem_limit_bytes=62 << 20, collective_id=1, has_side_effects=True),
        cost_estimate=pl.CostEstimate(flops=40_000_000_000, bytes_accessed=70 << 20, transcendentals=0),
        name="block_b",
    )(h_a, h_b, p_a, peer_a, p_b, mask, scale, wq, wo, keys, values, router, idx, wg, wu, wd)


def swap(part):
    return part, lax.ppermute(part, 'tp', SWAP)


def decode_body(hidden, write_pos, enc_mask, expert_idx, self_keys, self_values, cross_keys, cross_values, rel_bias, norm_scale, w_query, w_key, w_value, w_out, w_cross_query, w_cross_out, dense_gate, dense_up, dense_down, router, exp_gate, exp_up, exp_down):
    order = (0, 2, 3, 4, 1)
    keys, values = jnp.transpose(self_keys, order), jnp.transpose(self_values, order)
    ckeys, cvalues = jnp.transpose(cross_keys, order), jnp.transpose(cross_values, order)
    pos = write_pos.reshape(1, -1)
    mask = enc_mask.T
    scale = jnp.transpose(norm_scale, (1, 0, 2))
    def hbm(*arrays):
        return [pltpu.with_memory_space_constraint(array, pltpu.HBM) for array in arrays]

    hidden, pos, scale, rel_bias, mask = hbm(hidden, pos, scale, rel_bias, mask)
    w_query, w_key, w_value, w_out, w_cross_query, w_cross_out = hbm(w_query, w_key, w_value, w_out, w_cross_query, w_cross_out)
    keys, values, ckeys, cvalues = hbm(keys, values, ckeys, cvalues)
    dense_gate, dense_up, dense_down, exp_gate, exp_up, exp_down = hbm(dense_gate, dense_up, dense_down, exp_gate, exp_up, exp_down)
    router_t, idx = hbm(router.T, expert_idx.reshape(1, -1))
    shared = (pos, scale, rel_bias, w_query, w_key, w_value, w_out, keys, values)
    cross = (mask, scale, w_cross_query, w_cross_out, ckeys, cvalues)
    p_a, *outs = self_call(0, 0, hidden, None, *shared, None)
    pair_a = swap(p_a)
    p_b, *outs = self_call(0, 1, hidden, None, *shared, outs)
    h_a, h_b, pd_b = block_a_call(hidden, *pair_a, p_b, *cross, dense_gate, dense_up, dense_down)
    pair_b = swap(pd_b)
    p_a, *outs = self_call(1, 0, h_a, None, *shared, outs)
    pair_a = swap(p_a)
    h_b, p_b, *outs = self_call(1, 1, h_b, pair_b, *shared, outs)
    h_all = block_b_call(h_a, h_b, *pair_a, p_b, *cross, router_t, idx, exp_gate, exp_up, exp_down, lax.axis_size('ep'))
    back = (0, 4, 1, 2, 3)
    return h_all, jnp.transpose(outs[0], back), jnp.transpose(outs[1], back)


def solution(mesh):
    batch = ('dp', 'ep')
    row_spec = P(batch, None)
    vec_spec = P(batch)
    cache_spec = P(None, batch, 'tp', None, None)
    col_spec = P(None, None, 'tp')
    out_rows = P(None, 'tp', None)
    in_specs = (row_spec, vec_spec, row_spec, vec_spec, cache_spec, cache_spec, cache_spec, cache_spec, P('tp', None), P(), col_spec, col_spec, col_spec, out_rows, col_spec, out_rows, P(None, 'tp'), P(None, 'tp'), P('tp', None), P(), P('ep', None, 'tp'), P('ep', None, 'tp'), P('ep', 'tp', None))
    out_specs = (row_spec, cache_spec, cache_spec)
    return jax.shard_map(decode_body, mesh=mesh, in_specs=in_specs, out_specs=out_specs, check_vma=False)
```

```python
import functools

import jax
import jax.numpy as jnp
from jax import lax
from jax.experimental import pallas as pl
from jax.experimental.pallas import tpu as pltpu
from jax.sharding import PartitionSpec as P

EPS = 1e-6
NEG_BIG = -1e9
F32 = jnp.float32
BF16 = jnp.bfloat16
CHUNKS = 2
SELF_LIMIT = 18 << 20
B_LIMIT = 62 << 20
VMEM_SPEC = pl.BlockSpec(memory_space=pltpu.VMEM)
HBM_SPEC = pl.BlockSpec(memory_space=pltpu.HBM)
SWAP = [(0, 1), (1, 0)]


def rms_norm(h_cur, scale):
    h_float = h_cur.astype(F32)
    inv_rms = lax.rsqrt(jnp.mean(h_float * h_float, axis=-1, keepdims=True) + EPS)
    return (h_float * inv_rms * scale).astype(BF16)


def project(normed, weight):
    return jnp.dot(normed, weight, preferred_element_type=F32)


def add_parts(h_cur, own, peer):
    total = (own.astype(F32) + peer.astype(F32)).astype(BF16)
    return (h_cur.astype(F32) + total.astype(F32)).astype(BF16)


def softmax_rows(scores):
    top = jnp.max(scores, axis=0, keepdims=True)
    weight = jnp.exp(scores - top)
    return weight / jnp.sum(weight, axis=0, keepdims=True)


class Refs:
    def __init__(self, names, refs):
        self.__dict__.update(zip(names, refs, strict=True))


WEIGHTS = ('wq', 'wk', 'wv', 'wo')


def self_kernel(layer, chunk, ahead_first, names, *refs):
    t = Refs(names, refs)
    ready = hasattr(t, 'k_ready')
    heads, slots, head_dim, tc = t.kbuf.shape
    lanes = pl.ds(chunk * tc, tc)
    small = [
        pltpu.make_async_copy(t.pos.at[:, lanes], t.pos_scr, t.small_sem.at[0]),
        pltpu.make_async_copy(t.scale.at[0], t.scale_scr, t.small_sem.at[1]),
        pltpu.make_async_copy(t.bias, t.bias_scr, t.small_sem.at[2]),
    ]
    if hasattr(t, 'h_scr'):
        small.append(pltpu.make_async_copy(t.h.at[lanes, :], t.h_scr, t.small_sem.at[3]))
    for copy in small:
        copy.start()
    weights = []
    if hasattr(t, 'wq_hbm'):
        weights = [pltpu.make_async_copy(getattr(t, name + '_hbm').at[layer], getattr(t, name), t.w_sem.at[i]) for i, name in enumerate(WEIGHTS)]
    for copy in weights[:3]:
        copy.start()

    def fetch(head):
        if ready:
            return []
        return [
            pltpu.make_async_copy(t.keys.at[layer, head, :, :, lanes], t.kbuf.at[head], t.k_sem.at[head]),
            pltpu.make_async_copy(t.values.at[layer, head, :, :, lanes], t.vbuf.at[head], t.v_sem.at[head]),
        ]

    def store_k(head):
        return pltpu.make_async_copy(t.kbuf.at[head], t.ko.at[layer, head, :, :, lanes], t.ko_sem.at[head])

    def store_v(head):
        return pltpu.make_async_copy(t.vbuf.at[head], t.vo.at[layer, head, :, :, lanes], t.vo_sem.at[head])

    results = []
    for copy in fetch(0):
        copy.start()
    for copy in small:
        copy.wait()
    h_cur = t.h_scr[...] if hasattr(t, 'h_scr') else t.h[...]
    if hasattr(t, 'own'):
        h_cur = add_parts(h_cur, t.own[...], t.peer[...])
        t.h_out_scr[...] = h_cur
        results.append(pltpu.make_async_copy(t.h_out_scr, t.h_out, t.o_sem.at[1]))
        results[0].start()
    x = rms_norm(h_cur, t.scale_scr[layer:layer + 1, :])
    pos = t.pos_scr[...]
    t.posb[...] = jnp.broadcast_to(pos.astype(F32), t.posb.shape).astype(BF16)
    t.hot[...] = (lax.broadcasted_iota(jnp.int32, t.hot.shape, 0) == pos).astype(F32)
    t.line_scr[...] = jnp.zeros_like(t.line_scr)
    t.line_scr[0:heads, 0:slots] = t.bias_scr[...]
    for copy in weights[:3]:
        copy.wait()
    for head in range(1, heads):
        for copy in fetch(head):
            copy.start()
    ahead = []
    if hasattr(t, 'next_k'):
        for c in range(t.k_ahead.shape[0]):
            cols = pl.ds((c + ahead_first) * tc, tc)
            ahead.append(pltpu.make_async_copy(t.next_k.at[1, :, :, :, cols], t.k_ahead.at[c], t.a_sem.at[2 * c]))
            ahead.append(pltpu.make_async_copy(t.next_v.at[1, :, :, :, cols], t.v_ahead.at[c], t.a_sem.at[2 * c + 1]))
    for copy in weights[3:] + ahead:
        copy.start()
    t.q_t[...] = jnp.transpose(project(x, t.wq[...])).astype(BF16).astype(F32)
    t.k_t[...] = jnp.transpose(project(x, t.wk[...])).astype(BF16)
    t.v_t[...] = jnp.transpose(project(x, t.wv[...])).astype(BF16)
    posv = t.posb[...]
    k_src, v_src = (t.k_ready.at[0], t.v_ready.at[0]) if ready else (t.kbuf, t.vbuf)

    @pl.loop(0, heads)
    def _(head):
        rows = pl.ds(pl.multiple_of(head * head_dim, head_dim), head_dim)
        q = t.q_t[rows, :]
        k_new = t.k_t[rows, :]
        arrive = fetch(head)
        for copy in arrive[:1]:
            copy.wait()
        for s8 in range(0, slots, 8):
            out_rows = []
            for s in range(s8, s8 + 8):
                cur = jnp.where(posv == jnp.asarray(s, BF16), k_new, k_src[head, s])
                t.kbuf[head, s] = cur
                out_rows.append(jnp.sum(cur.astype(F32) * q, axis=0, keepdims=True))
            t.prob[s8:s8 + 8, :] = jnp.concatenate(out_rows, axis=0)
        store_k(head).start()
        line = jnp.broadcast_to(t.line_scr[pl.ds(head, 1), :], (slots, 128))
        table = pltpu.roll(line, 0, 1, stride=1, stride_axis=0)
        bias = jnp.dot(table, t.hot[...], precision=lax.Precision.HIGHEST, preferred_element_type=F32)
        slot_id = lax.broadcasted_iota(jnp.int32, bias.shape, 0)
        scores = jnp.where(slot_id <= t.pos_scr[...], t.prob[...] + bias, NEG_BIG)
        t.prob[...] = softmax_rows(scores).astype(BF16).astype(F32)
        v_new = t.v_t[rows, :]
        for copy in arrive[1:]:
            copy.wait()
        acc = jnp.zeros(q.shape, F32)
        for s in range(slots):
            cur = jnp.where(posv == jnp.asarray(s, BF16), v_new, v_src[head, s])
            t.vbuf[head, s] = cur
            acc = acc + t.prob[s:s + 1, :] * cur.astype(F32)
        store_v(head).start()
        t.ctx_t[rows, :] = acc

    for copy in weights[3:]:
        copy.wait()
    ctx = jnp.transpose(t.ctx_t[...]).astype(BF16)
    t.part_scr[...] = project(ctx, t.wo[...]).astype(BF16)
    results.append(pltpu.make_async_copy(t.part_scr, t.part, t.o_sem.at[0]))
    results[-1].start()
    for head in range(heads):
        store_k(head).wait()
        store_v(head).wait()
    for copy in ahead + results:
        copy.wait()


def weight_shapes(dim, width):
    return [(dim, width)] * 3 + [(width, dim)]


def self_call(layer, chunk, h_cur, pos, scale, bias, keys, values, outs=None, parts=None, weights=None, held=None, ready=None, ahead=None, ahead_first=0):
    heads, slots, head_dim, tokens = keys.shape[1:]
    tc = tokens // CHUNKS
    dim = h_cur.shape[1]
    width = heads * head_dim
    args, specs, aliases, names, out_shape, out_names, out_specs = [], [], {}, [], [], [], []

    def take(spec, pairs):
        for name, array in pairs:
            names.append(name)
            args.append(array)
            specs.append(spec)

    def give(name, shape):
        out_names.append(name)
        out_shape.append(pltpu.VMEM(shape, BF16))
        out_specs.append(VMEM_SPEC)

    def result(name):
        out_names.append(name)
        out_shape.append(pltpu.HBM((tc, dim), BF16))
        out_specs.append(HBM_SPEC)

    take(HBM_SPEC if h_cur.shape[0] != tc else VMEM_SPEC, [('h', h_cur)])
    if parts is not None:
        take(VMEM_SPEC, zip(('own', 'peer'), parts))
        result('h_out')
    result('part')
    take(HBM_SPEC, (('pos', pos), ('scale', scale), ('bias', bias)))
    if weights is not None:
        take(HBM_SPEC, zip([name + '_hbm' for name in WEIGHTS], weights))
        for name, shape in zip(WEIGHTS, weight_shapes(dim, width)):
            give(name, shape)
    else:
        take(VMEM_SPEC, zip(WEIGHTS, held))
    if ready is None:
        take(HBM_SPEC, (('keys', keys), ('values', values)))
    else:
        take(VMEM_SPEC, zip(('k_ready', 'v_ready'), ready))
    if ahead is not None:
        take(HBM_SPEC, zip(('next_k', 'next_v'), ahead))
        shape = (CHUNKS - ahead_first, heads, ahead[0].shape[2], head_dim, tc)
        give('k_ahead', shape)
        give('v_ahead', shape)
    count = len(out_shape)
    if outs is not None:
        aliases = {len(args): count, len(args) + 1: count + 1}
        take(HBM_SPEC, zip(('old_k', 'old_v'), outs))
    out_shape += [jax.ShapeDtypeStruct(keys.shape, BF16)] * 2
    scratch = dict(
        pos_scr=pltpu.VMEM((1, tc), jnp.int32),
        scale_scr=pltpu.VMEM(scale.shape[1:], F32),
        bias_scr=pltpu.VMEM(bias.shape, F32),
        line_scr=pltpu.VMEM((8, 128), F32),
        kbuf=pltpu.VMEM((heads, slots, head_dim, tc), BF16),
        vbuf=pltpu.VMEM((heads, slots, head_dim, tc), BF16),
        q_t=pltpu.VMEM((width, tc), F32),
        k_t=pltpu.VMEM((width, tc), BF16),
        v_t=pltpu.VMEM((width, tc), BF16),
        ctx_t=pltpu.VMEM((width, tc), F32),
        prob=pltpu.VMEM((slots, tc), F32),
        posb=pltpu.VMEM((head_dim, tc), BF16),
        hot=pltpu.VMEM((128, tc), F32),
        part_scr=pltpu.VMEM((tc, dim), BF16),
        h_out_scr=pltpu.VMEM((tc, dim), BF16),
        o_sem=pltpu.SemaphoreType.DMA((2,)),
        small_sem=pltpu.SemaphoreType.DMA((4,)),
        w_sem=pltpu.SemaphoreType.DMA((4,)),
        a_sem=pltpu.SemaphoreType.DMA((4,)),
        k_sem=pltpu.SemaphoreType.DMA((heads,)),
        v_sem=pltpu.SemaphoreType.DMA((heads,)),
        ko_sem=pltpu.SemaphoreType.DMA((heads,)),
        vo_sem=pltpu.SemaphoreType.DMA((heads,)),
    )
    if h_cur.shape[0] != tc:
        scratch.update(h_scr=pltpu.VMEM((tc, dim), BF16))
    size = heads * slots * head_dim * tc
    return pl.pallas_call(
        functools.partial(self_kernel, layer, chunk, ahead_first, tuple(names + out_names + ['ko', 'vo'] + list(scratch))),
        in_specs=specs,
        out_specs=out_specs + [HBM_SPEC] * 2,
        out_shape=out_shape,
        input_output_aliases=aliases,
        scratch_shapes=list(scratch.values()),
        compiler_params=pltpu.CompilerParams(vmem_limit_bytes=SELF_LIMIT),
        cost_estimate=pl.CostEstimate(flops=size * 400, bytes_accessed=size * 8, transcendentals=0),
        name=f"self{layer}_{chunk}",
    )(*args)


def tp_peer():
    return (lax.axis_index('dp'), 1 - lax.axis_index('tp'), lax.axis_index('ep'))


def remote(src, dst, sems, device):
    return pltpu.make_async_remote_copy(src_ref=src, dst_ref=dst, send_sem=sems[0], recv_sem=sems[1], device_id=device, device_id_type=pl.DeviceIdType.MESH)


def greet(devices):
    barrier = pltpu.get_barrier_semaphore()
    for device in devices:
        pl.semaphore_signal(barrier, inc=1, device_id=device, device_id_type=pl.DeviceIdType.MESH)
    pl.semaphore_wait(barrier, len(devices))


def cross_part(x, keys, values, mask_t, wq, wo, q_t, ctx_t, prob, after_query, out_ref):
    heads, slots, head_dim, _ = keys.shape
    q_t[...] = jnp.transpose(project(x, wq[...])).astype(BF16).astype(F32)
    after_query()

    @pl.loop(0, heads)
    def _(head):
        rows = pl.ds(pl.multiple_of(head * head_dim, head_dim), head_dim)
        q = q_t[rows, :]
        for s8 in range(0, slots, 8):
            out_rows = []
            for s in range(s8, s8 + 8):
                out_rows.append(jnp.sum(keys[head, s].astype(F32) * q, axis=0, keepdims=True))
            prob[s8:s8 + 8, :] = jnp.concatenate(out_rows, axis=0)
        scores = jnp.where(mask_t > 0, prob[...], NEG_BIG)
        prob[...] = softmax_rows(scores).astype(BF16).astype(F32)
        acc = jnp.zeros(q.shape, F32)
        for s in range(slots):
            acc = acc + prob[s:s + 1, :] * values[head, s].astype(F32)
        ctx_t[rows, :] = acc

    ctx = jnp.transpose(ctx_t[...]).astype(BF16)
    out_ref[...] = project(ctx, wo[...]).astype(BF16)


def cross_scratch(heads, slots, head_dim, tokens, dim, caches, staged):
    tc = tokens // 2
    width = heads * head_dim
    kept = {}
    if caches:
        kept = {name: pltpu.VMEM((2, heads, slots, head_dim, tc), BF16) for name in ('kbuf', 'vbuf')}
        kept['kv_sem'] = pltpu.SemaphoreType.DMA((2, 2))
    return dict(
        **kept,
        staged=pltpu.VMEM((staged, tc, dim), BF16),
        st_sem=pltpu.SemaphoreType.DMA((staged,)),
        scale_scr=pltpu.VMEM((3, 2, dim), F32),
        mask_scr=pltpu.VMEM((slots, tokens), jnp.int32),
        wq_scr=pltpu.VMEM((dim, width), BF16),
        wo_scr=pltpu.VMEM((width, dim), BF16),
        q_t=pltpu.VMEM((width, tc), F32),
        ctx_t=pltpu.VMEM((width, tc), F32),
        prob=pltpu.VMEM((slots, tc), F32),
        sbuf=pltpu.VMEM((3, tc, dim), BF16),
        rbuf=pltpu.VMEM((4, tc, dim), BF16),
        send_sem=pltpu.SemaphoreType.DMA((4,)),
        recv_sem=pltpu.SemaphoreType.DMA((4,)),
        c_sem=pltpu.SemaphoreType.DMA((4,)),
    )


class Cross:
    def __init__(self, layer, r, t, count, staged):
        self.layer, self.r, self.t = layer, r, t
        self.rows = []
        self.send_row = staged.index('p_b')
        for i, name in enumerate(staged):
            self.rows.append(pltpu.make_async_copy(getattr(r, name), t.staged.at[i], t.st_sem.at[i]))
            setattr(r, name, t.staged.at[i])
        tc = t.sbuf.shape[1]
        self.loads = [
            pltpu.make_async_copy(r.scale, t.scale_scr, t.c_sem.at[0]),
            pltpu.make_async_copy(r.mask, t.mask_scr, t.c_sem.at[1]),
            pltpu.make_async_copy(r.wq.at[layer], t.wq_scr, t.c_sem.at[2]),
            pltpu.make_async_copy(r.wo.at[layer], t.wo_scr, t.c_sem.at[3]),
        ]
        self.caches = t.kbuf, t.vbuf
        peer = tp_peer()
        sources = [r.p_b] + [t.sbuf.at[i] for i in range(3)]
        self.swaps = [remote(sources[i], t.rbuf.at[i], (t.send_sem.at[i], t.recv_sem.at[i]), peer) for i in range(count)]
        self.tc = tc

    def kv(self, c):
        r, t, where = self.r, self.t, (self.layer, slice(None), slice(None), slice(None), pl.ds(c * self.tc, self.tc))
        return [
            pltpu.make_async_copy(r.keys.at[where], t.kbuf.at[c], t.kv_sem.at[c, 0]),
            pltpu.make_async_copy(r.values.at[where], t.vbuf.at[c], t.kv_sem.at[c, 1]),
        ]

    def start_kv(self, c):
        for copy in self.kv(c):
            copy.start()

    def start_loads(self):
        for copy in self.rows + self.loads[:4]:
            copy.start()
        self.start_kv(0)

    def run(self, later):
        t, r = self.t, self.r
        for copy in self.rows[self.send_row:self.send_row + 1]:
            copy.wait()
        self.swaps[0].start()
        for copy in self.rows[:self.send_row] + self.rows[self.send_row + 1:]:
            copy.wait()
        for copy in self.loads:
            copy.wait()
        self.start_kv(1)
        streams = []
        for c in range(2):
            if c == 0:
                h_cur = add_parts(r.h_a[...], r.p_a[...], r.peer_a[...])
            else:
                self.swaps[0].wait_recv()
                h_cur = add_parts(r.h_b[...], r.p_b[...], t.rbuf[0])
            streams.append(h_cur)
            x = rms_norm(h_cur, t.scale_scr[1, self.layer:self.layer + 1, :])

            def after_query():
                for copy in self.kv(c):
                    copy.wait()
                if c == 0:
                    for copy in later:
                        copy.start()

            cross_part(x, self.caches[0].at[c], self.caches[1].at[c], t.mask_scr[:, c * self.tc:(c + 1) * self.tc], t.wq_scr, t.wo_scr, t.q_t, t.ctx_t, t.prob, after_query, t.sbuf.at[c])
            self.swaps[1 + c].start()
        return streams


CROSS_IN = ('h_a', 'h_b', 'p_a', 'peer_a', 'p_b', 'mask', 'scale', 'wq', 'wo', 'keys', 'values')


def dense_part(x, wg, wu, wd, acc, out_ref, tile=512):
    acc[...] = jnp.zeros_like(acc)

    @pl.loop(0, wg.shape[1] // tile)
    def _(i):
        cols = pl.ds(pl.multiple_of(i * tile, tile), tile)
        product = (jax.nn.gelu(project(x, wg[:, cols])) * project(x, wu[:, cols])).astype(BF16)
        acc[...] += project(product, wd[cols, :])

    out_ref[...] = acc[...].astype(BF16)


def block_a_kernel(names, *refs):
    r = t = Refs(names, refs)
    stream = pltpu.make_async_copy(r.hidden, t.h_scr, t.d_sem.at[3])
    stream.start()
    tc = t.acc.shape[0]
    r.h_a, r.h_b = t.h_scr.at[0:tc, :], t.h_scr.at[tc:, :]
    cross = Cross(0, r, t, 4, ('p_a', 'peer_a', 'p_b'))
    cross.loads.append(stream)
    cross.start_loads()
    ahead = [pltpu.make_async_copy(getattr(r, name + '_next').at[1], getattr(r, name + '_out'), t.n_sem.at[i]) for i, name in enumerate(WEIGHTS)]
    for c, (k_out, v_out) in enumerate(((r.k_a.at[0], r.v_a.at[0]), (r.k_b.at[0], r.v_b.at[0]))):
        lanes = pl.ds(c * tc, tc)
        ahead.append(pltpu.make_async_copy(r.next_k.at[1, :, :, :, lanes], k_out, t.n_sem.at[4 + 2 * c]))
        ahead.append(pltpu.make_async_copy(r.next_v.at[1, :, :, :, lanes], v_out, t.n_sem.at[5 + 2 * c]))
    dense = [pltpu.make_async_copy(src, dst, t.d_sem.at[i]) for i, (src, dst) in enumerate(((r.wg, t.wg_scr), (r.wu, t.wu_scr), (r.wd, t.wd_scr)))]
    greet([tp_peer()])
    h_a, h_b = cross.run(dense)
    r.h2_a[...] = h_a
    r.h2_b[...] = h_b
    for copy in dense:
        copy.wait()
    for copy in ahead:
        copy.start()
    scale = t.scale_scr[2, 0:1, :]
    cross.swaps[1].wait_recv()
    h_a = add_parts(r.h2_a[...], t.sbuf[0], t.rbuf[1])
    r.h2_a[...] = h_a
    dense_part(rms_norm(h_a, scale), t.wg_scr, t.wu_scr, t.wd_scr, t.acc, t.sbuf.at[2])
    cross.swaps[3].start()
    cross.swaps[2].wait_recv()
    h_b = add_parts(r.h2_b[...], t.sbuf[1], t.rbuf[2])
    r.h2_b[...] = h_b
    dense_part(rms_norm(h_b, scale), t.wg_scr, t.wu_scr, t.wd_scr, t.acc, r.pd_b)
    cross.swaps[3].wait_recv()
    r.h2_a[...] = add_parts(r.h2_a[...], t.sbuf[2], t.rbuf[3])
    for copy in cross.swaps:
        copy.wait_send()
    for copy in ahead:
        copy.wait()


def block_a_call(hidden, p_a, peer_a, p_b, mask, scale, wq, wo, keys, values, wg, wu, wd, next_weights, self_keys, self_values):
    _, heads, slots, head_dim, tokens = keys.shape
    dim, ff = wg.shape
    tc = tokens // 2
    scratch = cross_scratch(heads, slots, head_dim, tokens, dim, True, 3)
    scratch.update(
        wg_scr=pltpu.VMEM((dim, ff), BF16),
        wu_scr=pltpu.VMEM((dim, ff), BF16),
        wd_scr=pltpu.VMEM((ff, dim), BF16),
        acc=pltpu.VMEM((tc, dim), F32),
        h_scr=pltpu.VMEM((tokens, dim), BF16),
        d_sem=pltpu.SemaphoreType.DMA((4,)),
        n_sem=pltpu.SemaphoreType.DMA((8,)),
    )
    names = ('hidden',) + CROSS_IN[2:] + ('wg', 'wu', 'wd') + tuple(name + '_next' for name in WEIGHTS) + ('next_k', 'next_v', 'h2_a', 'h2_b', 'pd_b') + tuple(name + '_out' for name in WEIGHTS) + ('k_a', 'v_a', 'k_b', 'v_b') + tuple(scratch)
    cache = (1,) + self_keys.shape[1:4] + (tc,)
    shapes = [(tc, dim)] * 3 + weight_shapes(dim, heads * head_dim) + [cache] * 4
    return pl.pallas_call(
        functools.partial(block_a_kernel, names),
        in_specs=[HBM_SPEC] * 19,
        out_specs=[VMEM_SPEC] * 11,
        out_shape=[pltpu.VMEM(shape, BF16) for shape in shapes],
        scratch_shapes=list(scratch.values()),
        compiler_params=pltpu.CompilerParams(vmem_limit_bytes=30 << 20, collective_id=0, has_side_effects=True),
        cost_estimate=pl.CostEstimate(flops=20_000_000_000, bytes_accessed=20 << 20, transcendentals=0),
        name="block_a",
    )(hidden, p_a, peer_a, p_b, mask, scale, wq, wo, keys, values, wg, wu, wd, *next_weights, self_keys, self_values)


def block_b_kernel(names, *refs):
    r = t = Refs(names, refs)
    dp, tp, me = lax.axis_index('dp'), lax.axis_index('tp'), lax.axis_index('ep')
    group = lax.axis_size('ep')
    local, cap_rows, dim = t.xin.shape
    capacity = cap_rows // group
    tokens = t.h_scr.shape[0]
    ring = t.wg_ring.shape[0]
    tc = tokens // 2
    half = dim // 2
    lag = 3
    rows_local = local * capacity
    near = (dp, tp, me + 1 - 2 * lax.rem(me, 2))
    across = (dp, tp, lax.rem(me + 2, group))
    others = [(dp, tp, lax.rem(me + k, group)) for k in range(1, group)]
    owners = (me, near[2], across[2], lax.rem(near[2] + 2, group))

    def fetch(i):
        slot = lax.rem(i, ring)
        return [pltpu.make_async_copy(src.at[i], dst.at[slot], t.e_sem.at[n, slot]) for n, (src, dst) in enumerate(((r.wg, t.wg_ring), (r.wu, t.wu_ring), (r.wd, t.wd_ring)))]

    cross = Cross(1, r, t, 3, ('p_b', 'p_a', 'peer_a', 'h_a', 'h_b'))
    cross.start_loads()
    side = [pltpu.make_async_copy(r.router, t.router_scr, t.s_sem.at[0]), pltpu.make_async_copy(r.idx, t.idx_scr, t.s_sem.at[1])]
    for copy in side:
        copy.start()
    greet([tp_peer()] + others)
    early = []
    for i in range(ring):
        early += fetch(i)

    h_a, h_b = cross.run(early)
    t.h_scr[0:tc, :] = h_a
    t.h_scr[tc:, :] = h_b
    def spread(c):
        rows = pl.ds(c * tc, tc)
        mine = t.x_scr.at[0, rows, :]
        return [
            remote(mine, t.x_scr.at[2, rows, :], (t.xs_sem.at[c, 0], t.xr_sem.at[c, 0]), across),
            remote(mine, t.x_scr.at[1, rows, :], (t.xs_sem.at[c, 1], t.xr_sem.at[c, 1]), near),
            remote(t.x_scr.at[2, rows, :], t.x_scr.at[3, rows, :], (t.xs_sem.at[c, 2], t.xr_sem.at[c, 2]), near),
        ]

    def span(owner, i):
        return pl.ds(pl.multiple_of((owner * local + i) * capacity, capacity), capacity)

    def mine(owner):
        return pl.ds(pl.multiple_of(owner * capacity, capacity), capacity)

    def send_back(i, k):
        dst = lax.rem(me + k, group)
        return remote(t.ysum.at[i, mine(dst), :], t.ret.at[span(me, i), :], (t.bs_sem.at[k - 1, i], t.br_sem.at[k - 1, i]), (dp, tp, dst))

    def fold(i):
        return remote(t.yout.at[i], t.yin.at[i], (t.os_sem.at[i], t.or_sem.at[i]), tp_peer())

    def give_back(i):
        fold(i).wait_recv()
        t.ysum[i] = (t.ysum[i].astype(F32) + t.yin[i].astype(F32)).astype(BF16)
        for k in range(1, group):
            send_back(i, k).start()
        t.ret[span(me, i), :] = t.ysum[i, mine(me), :]

    def finish(c):
        rows = slice(c * tc, (c + 1) * tc)
        cross.swaps[1 + c].wait_recv()
        h_cur = add_parts(t.h_scr[rows, :], t.sbuf[c], t.rbuf[1 + c])
        t.h_scr[rows, :] = h_cur
        t.x_scr[0, rows, :] = rms_norm(h_cur, t.scale_scr[2, 1:2, :])
        hops = spread(c)
        hops[0].start()
        hops[1].start()
        return hops

    first = finish(0)
    side[1].wait()
    lane_idx = jnp.broadcast_to(t.idx_scr[...].astype(F32), (tokens, tokens))
    row_idx = jnp.transpose(lane_idx)
    same = lane_idx == row_idx
    row_no = lax.broadcasted_iota(jnp.int32, same.shape, 0)
    lane_no = lax.broadcasted_iota(jnp.int32, same.shape, 1)
    lane_slot = jnp.sum(jnp.where(same & (row_no < lane_no), 1.0, 0.0), axis=0, keepdims=True)
    row_slot = jnp.sum(jnp.where(same & (lane_no < row_no), 1.0, 0.0), axis=1, keepdims=True)
    total = group * rows_local
    lane_dest = jnp.where(lane_slot < capacity, lane_idx[0:1, :] * capacity + lane_slot, -1.0)
    row_dest = jnp.where(row_slot < capacity, row_idx[:, 0:1] * capacity + row_slot, -1.0)
    t.dest[0] = jnp.broadcast_to(lane_dest, t.dest.shape[1:])
    dest_sends = [remote(t.dest.at[0], t.dest.at[k], (t.is_sem.at[k - 1], t.ir_sem.at[k - 1]), (dp, tp, owners[k])) for k in range(1, group)]
    for copy in dest_sends:
        copy.start()
    t.place[...] = (lax.broadcasted_iota(jnp.int32, (tokens, total), 1).astype(F32) == row_dest).astype(BF16)
    t.hot[...] = jnp.where(lax.broadcasted_iota(jnp.int32, t.hot.shape, 1).astype(F32) == row_idx[:, 0:1], 1.0, 0.0)

    second = finish(1)
    first[0].wait_recv()
    first[2].start()
    first_row = (me * rows_local).astype(F32)
    for k in range(group):
        if k:
            dest_sends[k - 1].wait_recv()
        wanted = lax.broadcasted_iota(jnp.int32, (rows_local, tokens), 0).astype(F32) + first_row
        t.pick[k] = (wanted == t.dest[k, 0:1, :]).astype(BF16)
    side[0].wait()
    logits = jnp.dot(t.x_scr[0].astype(F32), t.router_scr[...].T, precision=lax.Precision.HIGHEST, preferred_element_type=F32)
    top = jnp.max(logits, axis=-1, keepdims=True)
    weight = jnp.exp(logits - top)
    weight = weight / jnp.sum(weight, axis=-1, keepdims=True)
    t.gate[...] = jnp.broadcast_to(jnp.sum(t.hot[...] * weight, axis=-1, keepdims=True), t.gate.shape)
    second[0].wait_recv()
    second[2].start()
    for copy in first[1:] + second[1:]:
        copy.wait_recv()
    for k in range(group):
        block = project(t.pick[k], t.x_scr[k]).astype(BF16)
        for i in range(local):
            t.xin[i, mine(owners[k]), :] = block[i * capacity:(i + 1) * capacity, :]

    @pl.loop(0, local)
    def _(i):
        slot = lax.rem(i, ring)
        copies = fetch(i)
        x = t.xin[i]
        copies[0].wait()
        gate_in = jax.nn.gelu(project(x, t.wg_ring[slot]))
        copies[1].wait()
        product = (gate_in * project(x, t.wu_ring[slot])).astype(BF16)
        copies[2].wait()
        result = project(product, t.wd_ring[slot]).astype(BF16)
        low, high = result[:, :half], result[:, half:]
        t.ysum[i] = jnp.where(tp == 0, low, high)
        t.yout[i] = jnp.where(tp == 0, high, low)
        fold(i).start()

        @pl.when(i >= lag)
        def _():
            give_back(i - lag)

        @pl.when(i + ring < local)
        def _():
            for copy in fetch(i + ring):
                copy.start()

    @pl.loop(local - lag, local)
    def _(i):
        give_back(i)

    @pl.loop(0, local)
    def _(i):
        for k in range(1, group):
            send_back(i, k).wait_recv()

    pieces = t.comb.shape[0]
    size = tokens // pieces
    last = [remote(t.comb.at[p], t.comb_peer.at[p], (t.fs_sem.at[p], t.fr_sem.at[p]), tp_peer()) for p in range(pieces)]
    for p in range(pieces):
        t.comb[p] = project(t.place[p * size:(p + 1) * size, :], t.ret[...]).astype(BF16)
        last[p].start()
    for p in range(pieces):
        rows = slice(p * size, (p + 1) * size)
        last[p].wait_recv()
        own, peer = t.comb[p].astype(F32), t.comb_peer[p].astype(F32)
        gate = t.gate[rows, 0:1]
        for side_no, both in enumerate((jnp.where(tp == 0, own, peer), jnp.where(tp == 0, peer, own))):
            cols = slice(side_no * half, (side_no + 1) * half)
            r.out[rows, cols] = (t.h_scr[rows, cols].astype(F32) + gate * both).astype(BF16)
    for copy in cross.swaps + last + dest_sends + first + second:
        copy.wait_send()

    @pl.loop(0, local)
    def _(i):
        fold(i).wait_send()
        for k in range(1, group):
            send_back(i, k).wait_send()


def block_b_call(h_a, h_b, p_a, peer_a, p_b, mask, scale, wq, wo, keys, values, router, idx, wg, wu, wd, group):
    _, heads, slots, head_dim, tokens = keys.shape
    local, dim, ff = wg.shape
    experts = router.shape[0]
    capacity = (2 * tokens + experts - 1) // experts
    ring = 5
    pieces = 4
    scratch = cross_scratch(heads, slots, head_dim, tokens, dim, True, 5)
    hops = (group - 1, local)
    scratch.update(
        wg_ring=pltpu.VMEM((ring, dim, ff), BF16),
        wu_ring=pltpu.VMEM((ring, dim, ff), BF16),
        wd_ring=pltpu.VMEM((ring, ff, dim), BF16),
        router_scr=pltpu.VMEM(router.shape, F32),
        idx_scr=pltpu.VMEM((1, tokens), jnp.int32),
        h_scr=pltpu.VMEM((tokens, dim), BF16),
        x_scr=pltpu.VMEM((group, tokens, dim), BF16),
        dest=pltpu.VMEM((group, 8, tokens), F32),
        hot=pltpu.VMEM((tokens, experts), F32),
        pick=pltpu.VMEM((group, local * capacity, tokens), BF16),
        place=pltpu.VMEM((tokens, experts * capacity), BF16),
        gate=pltpu.VMEM((tokens, 128), F32),
        xin=pltpu.VMEM((local, group * capacity, dim), BF16),
        yout=pltpu.VMEM((local, group * capacity, dim // 2), BF16),
        yin=pltpu.VMEM((local, group * capacity, dim // 2), BF16),
        ysum=pltpu.VMEM((local, group * capacity, dim // 2), BF16),
        ret=pltpu.VMEM((experts * capacity, dim // 2), BF16),
        comb=pltpu.VMEM((pieces, tokens // pieces, dim // 2), BF16),
        comb_peer=pltpu.VMEM((pieces, tokens // pieces, dim // 2), BF16),
        e_sem=pltpu.SemaphoreType.DMA((3, ring)),
        s_sem=pltpu.SemaphoreType.DMA((2,)),
        is_sem=pltpu.SemaphoreType.DMA((group - 1,)),
        ir_sem=pltpu.SemaphoreType.DMA((group - 1,)),
        xs_sem=pltpu.SemaphoreType.DMA((2, 3)),
        xr_sem=pltpu.SemaphoreType.DMA((2, 3)),
        bs_sem=pltpu.SemaphoreType.DMA(hops),
        br_sem=pltpu.SemaphoreType.DMA(hops),
        os_sem=pltpu.SemaphoreType.DMA((local,)),
        or_sem=pltpu.SemaphoreType.DMA((local,)),
        fs_sem=pltpu.SemaphoreType.DMA((pieces,)),
        fr_sem=pltpu.SemaphoreType.DMA((pieces,)),
    )
    names = CROSS_IN + ('router', 'idx', 'wg', 'wu', 'wd', 'out') + tuple(scratch)
    return pl.pallas_call(
        functools.partial(block_b_kernel, names),
        in_specs=[HBM_SPEC] * 16,
        out_specs=VMEM_SPEC,
        out_shape=jax.ShapeDtypeStruct((tokens, dim), BF16),
        scratch_shapes=list(scratch.values()),
        compiler_params=pltpu.CompilerParams(vmem_limit_bytes=B_LIMIT, collective_id=1, has_side_effects=True),
        cost_estimate=pl.CostEstimate(flops=40_000_000_000, bytes_accessed=70 << 20, transcendentals=0),
        name="block_b",
    )(h_a, h_b, p_a, peer_a, p_b, mask, scale, wq, wo, keys, values, router, idx, wg, wu, wd)


def swap(part):
    return part, lax.ppermute(part, 'tp', SWAP)


def decode_body(hidden, write_pos, enc_mask, expert_idx, self_keys, self_values, cross_keys, cross_values, rel_bias, norm_scale, w_query, w_key, w_value, w_out, w_cross_query, w_cross_out, dense_gate, dense_up, dense_down, router, exp_gate, exp_up, exp_down):
    order = (0, 2, 3, 4, 1)
    keys, values = jnp.transpose(self_keys, order), jnp.transpose(self_values, order)
    ckeys, cvalues = jnp.transpose(cross_keys, order), jnp.transpose(cross_values, order)
    pos = write_pos.reshape(1, -1)
    mask = enc_mask.T
    scale = jnp.transpose(norm_scale, (1, 0, 2))
    def hbm(*arrays):
        return [pltpu.with_memory_space_constraint(array, pltpu.HBM) for array in arrays]

    hidden, pos, scale, rel_bias, mask = hbm(hidden, pos, scale, rel_bias, mask)
    w_query, w_key, w_value, w_out, w_cross_query, w_cross_out = hbm(w_query, w_key, w_value, w_out, w_cross_query, w_cross_out)
    keys, values, ckeys, cvalues = hbm(keys, values, ckeys, cvalues)
    dense_gate, dense_up, dense_down, exp_gate, exp_up, exp_down = hbm(dense_gate, dense_up, dense_down, exp_gate, exp_up, exp_down)
    router_t, idx = hbm(router.T, expert_idx.reshape(1, -1))
    shared = (pos, scale, rel_bias, keys, values)
    weights = (w_query, w_key, w_value, w_out)
    cross = (mask, scale, w_cross_query, w_cross_out, ckeys, cvalues)
    p_a, *rest = self_call(0, 0, hidden, *shared, weights=weights)
    held, outs = rest[:4], rest[4:]
    pair_a = swap(p_a)
    p_b, *outs = self_call(0, 1, hidden, *shared, outs=outs, held=held)
    h_a, h_b, pd_b, *rest = block_a_call(hidden, *pair_a, p_b, *cross, dense_gate, dense_up, dense_down, weights, keys, values)
    held, ready_a, ready_b = rest[:4], rest[4:6], rest[6:]
    pair_b = swap(pd_b)
    p_a, *outs = self_call(1, 0, h_a, *shared, outs=outs, held=held, ready=ready_a)
    pair_a = swap(p_a)
    h_b, p_b, *outs = self_call(1, 1, h_b, *shared, outs=outs, parts=pair_b, held=held, ready=ready_b)
    h_all = block_b_call(h_a, h_b, *pair_a, p_b, *cross, router_t, idx, exp_gate, exp_up, exp_down, lax.axis_size('ep'))
    back = (0, 4, 1, 2, 3)
    return h_all, jnp.transpose(outs[0], back), jnp.transpose(outs[1], back)


def solution(mesh):
    batch = ('dp', 'ep')
    row_spec = P(batch, None)
    vec_spec = P(batch)
    cache_spec = P(None, batch, 'tp', None, None)
    col_spec = P(None, None, 'tp')
    out_rows = P(None, 'tp', None)
    in_specs = (row_spec, vec_spec, row_spec, vec_spec, cache_spec, cache_spec, cache_spec, cache_spec, P('tp', None), P(), col_spec, col_spec, col_spec, out_rows, col_spec, out_rows, P(None, 'tp'), P(None, 'tp'), P('tp', None), P(), P('ep', None, 'tp'), P('ep', None, 'tp'), P('ep', 'tp', None))
    out_specs = (row_spec, cache_spec, cache_spec)
    return jax.shard_map(decode_body, mesh=mesh, in_specs=in_specs, out_specs=out_specs, check_vma=False)
```

```python
import functools

import jax
import jax.numpy as jnp
from jax import lax
from jax.experimental import pallas as pl
from jax.experimental.pallas import tpu as pltpu
from jax.sharding import PartitionSpec as P

EPS = 1e-6
NEG_BIG = -1e9
F32 = jnp.float32
BF16 = jnp.bfloat16
CHUNKS = 2
SELF_LIMIT = 18 << 20
B_LIMIT = 62 << 20
VMEM_SPEC = pl.BlockSpec(memory_space=pltpu.VMEM)
HBM_SPEC = pl.BlockSpec(memory_space=pltpu.HBM)
SWAP = [(0, 1), (1, 0)]


def rms_norm(h_cur, scale):
    h_float = h_cur.astype(F32)
    inv_rms = lax.rsqrt(jnp.mean(h_float * h_float, axis=-1, keepdims=True) + EPS)
    return (h_float * inv_rms * scale).astype(BF16)


def project(normed, weight):
    return jnp.dot(normed, weight, preferred_element_type=F32)


def add_parts(h_cur, own, peer):
    total = (own.astype(F32) + peer.astype(F32)).astype(BF16)
    return (h_cur.astype(F32) + total.astype(F32)).astype(BF16)


def softmax_rows(scores):
    top = jnp.max(scores, axis=0, keepdims=True)
    weight = jnp.exp(scores - top)
    return weight / jnp.sum(weight, axis=0, keepdims=True)


class Refs:
    def __init__(self, names, refs):
        self.__dict__.update(zip(names, refs, strict=True))


WEIGHTS = ('wq', 'wk', 'wv', 'wo')


def self_kernel(layer, chunk, ahead_first, names, *refs):
    t = Refs(names, refs)
    ready = hasattr(t, 'k_ready')
    heads, slots, head_dim, tc = t.kbuf.shape
    lanes = pl.ds(chunk * tc, tc)
    small = [
        pltpu.make_async_copy(t.pos.at[:, lanes], t.pos_scr, t.small_sem.at[0]),
        pltpu.make_async_copy(t.scale.at[0], t.scale_scr, t.small_sem.at[1]),
        pltpu.make_async_copy(t.bias, t.bias_scr, t.small_sem.at[2]),
    ]
    if hasattr(t, 'h_scr'):
        small.append(pltpu.make_async_copy(t.h.at[lanes, :], t.h_scr, t.small_sem.at[3]))
    for copy in small:
        copy.start()
    weights = []
    if hasattr(t, 'wq_hbm'):
        weights = [pltpu.make_async_copy(getattr(t, name + '_hbm').at[layer], getattr(t, name), t.w_sem.at[i]) for i, name in enumerate(WEIGHTS)]
    for copy in weights[:3]:
        copy.start()

    def fetch(head):
        if ready:
            return []
        return [
            pltpu.make_async_copy(t.keys.at[layer, head, :, :, lanes], t.kbuf.at[head], t.k_sem.at[head]),
            pltpu.make_async_copy(t.values.at[layer, head, :, :, lanes], t.vbuf.at[head], t.v_sem.at[head]),
        ]

    def store_k(head):
        return pltpu.make_async_copy(t.kbuf.at[head], t.ko.at[layer, head, :, :, lanes], t.ko_sem.at[head])

    def store_v(head):
        return pltpu.make_async_copy(t.vbuf.at[head], t.vo.at[layer, head, :, :, lanes], t.vo_sem.at[head])

    results = []
    for copy in fetch(0):
        copy.start()
    for copy in small:
        copy.wait()
    h_cur = t.h_scr[...] if hasattr(t, 'h_scr') else t.h[...]
    if hasattr(t, 'own'):
        h_cur = add_parts(h_cur, t.own[...], t.peer[...])
        t.h_out_scr[...] = h_cur
        results.append(pltpu.make_async_copy(t.h_out_scr, t.h_out, t.o_sem.at[1]))
        results[0].start()
    x = rms_norm(h_cur, t.scale_scr[layer:layer + 1, :])
    pos = t.pos_scr[...]
    t.posb[...] = jnp.broadcast_to(pos.astype(F32), t.posb.shape).astype(BF16)
    t.hot[...] = (lax.broadcasted_iota(jnp.int32, t.hot.shape, 0) == pos).astype(F32)
    t.line_scr[...] = jnp.zeros_like(t.line_scr)
    t.line_scr[0:heads, 0:slots] = t.bias_scr[...]
    for copy in weights[:3]:
        copy.wait()
    for head in range(1, heads):
        for copy in fetch(head):
            copy.start()
    ahead = []
    if hasattr(t, 'next_k'):
        for c in range(t.k_ahead.shape[0]):
            cols = pl.ds((c + ahead_first) * tc, tc)
            ahead.append(pltpu.make_async_copy(t.next_k.at[1, :, :, :, cols], t.k_ahead.at[c], t.a_sem.at[2 * c]))
            ahead.append(pltpu.make_async_copy(t.next_v.at[1, :, :, :, cols], t.v_ahead.at[c], t.a_sem.at[2 * c + 1]))
    for copy in weights[3:] + ahead:
        copy.start()
    t.q_t[...] = jnp.transpose(project(x, t.wq[...])).astype(BF16).astype(F32)
    t.k_t[...] = jnp.transpose(project(x, t.wk[...])).astype(BF16)
    t.v_t[...] = jnp.transpose(project(x, t.wv[...])).astype(BF16)
    posv = t.posb[...]
    k_src, v_src = (t.k_ready.at[0], t.v_ready.at[0]) if ready else (t.kbuf, t.vbuf)

    @pl.loop(0, heads)
    def _(head):
        rows = pl.ds(pl.multiple_of(head * head_dim, head_dim), head_dim)
        q = t.q_t[rows, :]
        k_new = t.k_t[rows, :]
        arrive = fetch(head)
        for copy in arrive[:1]:
            copy.wait()
        for s8 in range(0, slots, 8):
            out_rows = []
            for s in range(s8, s8 + 8):
                cur = jnp.where(posv == jnp.asarray(s, BF16), k_new, k_src[head, s])
                t.kbuf[head, s] = cur
                out_rows.append(jnp.sum(cur.astype(F32) * q, axis=0, keepdims=True))
            t.prob[s8:s8 + 8, :] = jnp.concatenate(out_rows, axis=0)
        store_k(head).start()
        line = jnp.broadcast_to(t.line_scr[pl.ds(head, 1), :], (slots, 128))
        table = pltpu.roll(line, 0, 1, stride=1, stride_axis=0)
        bias = jnp.dot(table, t.hot[...], precision=lax.Precision.HIGHEST, preferred_element_type=F32)
        slot_id = lax.broadcasted_iota(jnp.int32, bias.shape, 0)
        scores = jnp.where(slot_id <= t.pos_scr[...], t.prob[...] + bias, NEG_BIG)
        t.prob[...] = softmax_rows(scores).astype(BF16).astype(F32)
        v_new = t.v_t[rows, :]
        for copy in arrive[1:]:
            copy.wait()
        acc = jnp.zeros(q.shape, F32)
        for s in range(slots):
            cur = jnp.where(posv == jnp.asarray(s, BF16), v_new, v_src[head, s])
            t.vbuf[head, s] = cur
            acc = acc + t.prob[s:s + 1, :] * cur.astype(F32)
        store_v(head).start()
        t.ctx_t[rows, :] = acc

    for copy in weights[3:]:
        copy.wait()
    ctx = jnp.transpose(t.ctx_t[...]).astype(BF16)
    t.part_scr[...] = project(ctx, t.wo[...]).astype(BF16)
    results.append(pltpu.make_async_copy(t.part_scr, t.part, t.o_sem.at[0]))
    results[-1].start()
    for head in range(heads):
        store_k(head).wait()
        store_v(head).wait()
    for copy in ahead + results:
        copy.wait()


def weight_shapes(dim, width):
    return [(dim, width)] * 3 + [(width, dim)]


def self_call(layer, chunk, h_cur, pos, scale, bias, keys, values, outs=None, parts=None, weights=None, held=None, ready=None, ahead=None, ahead_first=0):
    heads, slots, head_dim, tokens = keys.shape[1:]
    tc = tokens // CHUNKS
    dim = h_cur.shape[1]
    width = heads * head_dim
    args, specs, aliases, names, out_shape, out_names, out_specs = [], [], {}, [], [], [], []

    def take(spec, pairs):
        for name, array in pairs:
            names.append(name)
            args.append(array)
            specs.append(spec)

    def give(name, shape):
        out_names.append(name)
        out_shape.append(pltpu.VMEM(shape, BF16))
        out_specs.append(VMEM_SPEC)

    def result(name):
        out_names.append(name)
        out_shape.append(pltpu.HBM((tc, dim), BF16))
        out_specs.append(HBM_SPEC)

    take(HBM_SPEC if h_cur.shape[0] != tc else VMEM_SPEC, [('h', h_cur)])
    if parts is not None:
        take(VMEM_SPEC, zip(('own', 'peer'), parts))
        result('h_out')
    result('part')
    take(HBM_SPEC, (('pos', pos), ('scale', scale), ('bias', bias)))
    if weights is not None:
        take(HBM_SPEC, zip([name + '_hbm' for name in WEIGHTS], weights))
        for name, shape in zip(WEIGHTS, weight_shapes(dim, width)):
            give(name, shape)
    else:
        take(VMEM_SPEC, zip(WEIGHTS, held))
    if ready is None:
        take(HBM_SPEC, (('keys', keys), ('values', values)))
    else:
        take(VMEM_SPEC, zip(('k_ready', 'v_ready'), ready))
    if ahead is not None:
        take(HBM_SPEC, zip(('next_k', 'next_v'), ahead))
        shape = (CHUNKS - ahead_first, heads, ahead[0].shape[2], head_dim, tc)
        give('k_ahead', shape)
        give('v_ahead', shape)
    count = len(out_shape)
    if outs is not None:
        aliases = {len(args): count, len(args) + 1: count + 1}
        take(HBM_SPEC, zip(('old_k', 'old_v'), outs))
    out_shape += [jax.ShapeDtypeStruct(keys.shape, BF16)] * 2
    scratch = dict(
        pos_scr=pltpu.VMEM((1, tc), jnp.int32),
        scale_scr=pltpu.VMEM(scale.shape[1:], F32),
        bias_scr=pltpu.VMEM(bias.shape, F32),
        line_scr=pltpu.VMEM((8, 128), F32),
        kbuf=pltpu.VMEM((heads, slots, head_dim, tc), BF16),
        vbuf=pltpu.VMEM((heads, slots, head_dim, tc), BF16),
        q_t=pltpu.VMEM((width, tc), F32),
        k_t=pltpu.VMEM((width, tc), BF16),
        v_t=pltpu.VMEM((width, tc), BF16),
        ctx_t=pltpu.VMEM((width, tc), F32),
        prob=pltpu.VMEM((slots, tc), F32),
        posb=pltpu.VMEM((head_dim, tc), BF16),
        hot=pltpu.VMEM((128, tc), F32),
        part_scr=pltpu.VMEM((tc, dim), BF16),
        h_out_scr=pltpu.VMEM((tc, dim), BF16),
        o_sem=pltpu.SemaphoreType.DMA((2,)),
        small_sem=pltpu.SemaphoreType.DMA((4,)),
        w_sem=pltpu.SemaphoreType.DMA((4,)),
        a_sem=pltpu.SemaphoreType.DMA((4,)),
        k_sem=pltpu.SemaphoreType.DMA((heads,)),
        v_sem=pltpu.SemaphoreType.DMA((heads,)),
        ko_sem=pltpu.SemaphoreType.DMA((heads,)),
        vo_sem=pltpu.SemaphoreType.DMA((heads,)),
    )
    if h_cur.shape[0] != tc:
        scratch.update(h_scr=pltpu.VMEM((tc, dim), BF16))
    size = heads * slots * head_dim * tc
    return pl.pallas_call(
        functools.partial(self_kernel, layer, chunk, ahead_first, tuple(names + out_names + ['ko', 'vo'] + list(scratch))),
        in_specs=specs,
        out_specs=out_specs + [HBM_SPEC] * 2,
        out_shape=out_shape,
        input_output_aliases=aliases,
        scratch_shapes=list(scratch.values()),
        compiler_params=pltpu.CompilerParams(vmem_limit_bytes=SELF_LIMIT),
        cost_estimate=pl.CostEstimate(flops=size * 400, bytes_accessed=size * 8, transcendentals=0),
        name=f"self{layer}_{chunk}",
    )(*args)


def tp_peer():
    return (lax.axis_index('dp'), 1 - lax.axis_index('tp'), lax.axis_index('ep'))


def remote(src, dst, sems, device):
    return pltpu.make_async_remote_copy(src_ref=src, dst_ref=dst, send_sem=sems[0], recv_sem=sems[1], device_id=device, device_id_type=pl.DeviceIdType.MESH)


def greet(devices):
    barrier = pltpu.get_barrier_semaphore()
    for device in devices:
        pl.semaphore_signal(barrier, inc=1, device_id=device, device_id_type=pl.DeviceIdType.MESH)
    pl.semaphore_wait(barrier, len(devices))


def cross_part(x, keys, values, mask_t, wq, wo, q_t, ctx_t, prob, after_query, out_ref):
    heads, slots, head_dim, _ = keys.shape
    q_t[...] = jnp.transpose(project(x, wq[...])).astype(BF16).astype(F32)
    after_query()

    @pl.loop(0, heads)
    def _(head):
        rows = pl.ds(pl.multiple_of(head * head_dim, head_dim), head_dim)
        q = q_t[rows, :]
        for s8 in range(0, slots, 8):
            out_rows = []
            for s in range(s8, s8 + 8):
                out_rows.append(jnp.sum(keys[head, s].astype(F32) * q, axis=0, keepdims=True))
            prob[s8:s8 + 8, :] = jnp.concatenate(out_rows, axis=0)
        scores = jnp.where(mask_t > 0, prob[...], NEG_BIG)
        prob[...] = softmax_rows(scores).astype(BF16).astype(F32)
        acc = jnp.zeros(q.shape, F32)
        for s in range(slots):
            acc = acc + prob[s:s + 1, :] * values[head, s].astype(F32)
        ctx_t[rows, :] = acc

    ctx = jnp.transpose(ctx_t[...]).astype(BF16)
    out_ref[...] = project(ctx, wo[...]).astype(BF16)


def cross_scratch(heads, slots, head_dim, tokens, dim, caches, staged):
    tc = tokens // 2
    width = heads * head_dim
    kept = {}
    if caches:
        kept = {name: pltpu.VMEM((2, heads, slots, head_dim, tc), BF16) for name in ('kbuf', 'vbuf')}
        kept['kv_sem'] = pltpu.SemaphoreType.DMA((2, 2))
    return dict(
        **kept,
        staged=pltpu.VMEM((staged, tc, dim), BF16),
        st_sem=pltpu.SemaphoreType.DMA((staged,)),
        scale_scr=pltpu.VMEM((3, 2, dim), F32),
        mask_scr=pltpu.VMEM((slots, tokens), jnp.int32),
        wq_scr=pltpu.VMEM((dim, width), BF16),
        wo_scr=pltpu.VMEM((width, dim), BF16),
        q_t=pltpu.VMEM((width, tc), F32),
        ctx_t=pltpu.VMEM((width, tc), F32),
        prob=pltpu.VMEM((slots, tc), F32),
        sbuf=pltpu.VMEM((3, tc, dim), BF16),
        rbuf=pltpu.VMEM((4, tc, dim), BF16),
        send_sem=pltpu.SemaphoreType.DMA((4,)),
        recv_sem=pltpu.SemaphoreType.DMA((4,)),
        c_sem=pltpu.SemaphoreType.DMA((4,)),
    )


class Cross:
    def __init__(self, layer, r, t, count, staged):
        self.layer, self.r, self.t = layer, r, t
        self.rows = []
        self.send_row = staged.index('p_b')
        for i, name in enumerate(staged):
            self.rows.append(pltpu.make_async_copy(getattr(r, name), t.staged.at[i], t.st_sem.at[i]))
            setattr(r, name, t.staged.at[i])
        tc = t.sbuf.shape[1]
        self.loads = [
            pltpu.make_async_copy(r.scale, t.scale_scr, t.c_sem.at[0]),
            pltpu.make_async_copy(r.mask, t.mask_scr, t.c_sem.at[1]),
            pltpu.make_async_copy(r.wq.at[layer], t.wq_scr, t.c_sem.at[2]),
            pltpu.make_async_copy(r.wo.at[layer], t.wo_scr, t.c_sem.at[3]),
        ]
        self.caches = t.kbuf, t.vbuf
        peer = tp_peer()
        sources = [r.p_b] + [t.sbuf.at[i] for i in range(3)]
        self.swaps = [remote(sources[i], t.rbuf.at[i], (t.send_sem.at[i], t.recv_sem.at[i]), peer) for i in range(count)]
        self.tc = tc

    def kv(self, c):
        r, t, where = self.r, self.t, (self.layer, slice(None), slice(None), slice(None), pl.ds(c * self.tc, self.tc))
        return [
            pltpu.make_async_copy(r.keys.at[where], t.kbuf.at[c], t.kv_sem.at[c, 0]),
            pltpu.make_async_copy(r.values.at[where], t.vbuf.at[c], t.kv_sem.at[c, 1]),
        ]

    def start_kv(self, c):
        for copy in self.kv(c):
            copy.start()

    def start_loads(self):
        for copy in self.rows + self.loads[:4]:
            copy.start()
        self.start_kv(0)

    def run(self, later):
        t, r = self.t, self.r
        for copy in self.rows[self.send_row:self.send_row + 1]:
            copy.wait()
        self.swaps[0].start()
        for copy in self.rows[:self.send_row] + self.rows[self.send_row + 1:]:
            copy.wait()
        for copy in self.loads:
            copy.wait()
        self.start_kv(1)
        streams = []
        for c in range(2):
            if c == 0:
                h_cur = add_parts(r.h_a[...], r.p_a[...], r.peer_a[...])
            else:
                self.swaps[0].wait_recv()
                h_cur = add_parts(r.h_b[...], r.p_b[...], t.rbuf[0])
            streams.append(h_cur)
            x = rms_norm(h_cur, t.scale_scr[1, self.layer:self.layer + 1, :])

            def after_query():
                for copy in self.kv(c):
                    copy.wait()
                if c == 0:
                    for copy in later:
                        copy.start()

            cross_part(x, self.caches[0].at[c], self.caches[1].at[c], t.mask_scr[:, c * self.tc:(c + 1) * self.tc], t.wq_scr, t.wo_scr, t.q_t, t.ctx_t, t.prob, after_query, t.sbuf.at[c])
            self.swaps[1 + c].start()
        return streams


CROSS_IN = ('h_a', 'h_b', 'p_a', 'peer_a', 'p_b', 'mask', 'scale', 'wq', 'wo', 'keys', 'values')


def dense_part(x, wg, wu, wd, acc, out_ref, tile=512):
    acc[...] = jnp.zeros_like(acc)

    @pl.loop(0, wg.shape[1] // tile)
    def _(i):
        cols = pl.ds(pl.multiple_of(i * tile, tile), tile)
        product = (jax.nn.gelu(project(x, wg[:, cols])) * project(x, wu[:, cols])).astype(BF16)
        acc[...] += project(product, wd[cols, :])

    out_ref[...] = acc[...].astype(BF16)


def block_a_kernel(names, *refs):
    r = t = Refs(names, refs)
    stream = pltpu.make_async_copy(r.hidden, t.h_scr, t.d_sem.at[3])
    stream.start()
    tc = t.acc.shape[0]
    r.h_a, r.h_b = t.h_scr.at[0:tc, :], t.h_scr.at[tc:, :]
    cross = Cross(0, r, t, 4, ('p_a', 'peer_a', 'p_b'))
    cross.loads.append(stream)
    cross.start_loads()
    ahead = [pltpu.make_async_copy(getattr(r, name + '_next').at[1], getattr(r, name + '_out'), t.n_sem.at[i]) for i, name in enumerate(WEIGHTS)]
    for c, (k_out, v_out) in enumerate(((r.k_a.at[0], r.v_a.at[0]), (r.k_b.at[0], r.v_b.at[0]))):
        lanes = pl.ds(c * tc, tc)
        ahead.append(pltpu.make_async_copy(r.next_k.at[1, :, :, :, lanes], k_out, t.n_sem.at[4 + 2 * c]))
        ahead.append(pltpu.make_async_copy(r.next_v.at[1, :, :, :, lanes], v_out, t.n_sem.at[5 + 2 * c]))
    dense = [pltpu.make_async_copy(src, dst, t.d_sem.at[i]) for i, (src, dst) in enumerate(((r.wg, t.wg_scr), (r.wu, t.wu_scr), (r.wd, t.wd_scr)))]
    greet([tp_peer()])
    h_a, h_b = cross.run(dense)
    r.h2_a[...] = h_a
    r.h2_b[...] = h_b
    for copy in dense:
        copy.wait()
    for copy in ahead:
        copy.start()
    scale = t.scale_scr[2, 0:1, :]
    cross.swaps[1].wait_recv()
    h_a = add_parts(r.h2_a[...], t.sbuf[0], t.rbuf[1])
    r.h2_a[...] = h_a
    dense_part(rms_norm(h_a, scale), t.wg_scr, t.wu_scr, t.wd_scr, t.acc, t.sbuf.at[2])
    cross.swaps[3].start()
    cross.swaps[2].wait_recv()
    h_b = add_parts(r.h2_b[...], t.sbuf[1], t.rbuf[2])
    r.h2_b[...] = h_b
    dense_part(rms_norm(h_b, scale), t.wg_scr, t.wu_scr, t.wd_scr, t.acc, r.pd_b)
    cross.swaps[3].wait_recv()
    r.h2_a[...] = add_parts(r.h2_a[...], t.sbuf[2], t.rbuf[3])
    for copy in cross.swaps:
        copy.wait_send()
    for copy in ahead:
        copy.wait()


def block_a_call(hidden, p_a, peer_a, p_b, mask, scale, wq, wo, keys, values, wg, wu, wd, next_weights, self_keys, self_values):
    _, heads, slots, head_dim, tokens = keys.shape
    dim, ff = wg.shape
    tc = tokens // 2
    scratch = cross_scratch(heads, slots, head_dim, tokens, dim, True, 3)
    scratch.update(
        wg_scr=pltpu.VMEM((dim, ff), BF16),
        wu_scr=pltpu.VMEM((dim, ff), BF16),
        wd_scr=pltpu.VMEM((ff, dim), BF16),
        acc=pltpu.VMEM((tc, dim), F32),
        h_scr=pltpu.VMEM((tokens, dim), BF16),
        d_sem=pltpu.SemaphoreType.DMA((4,)),
        n_sem=pltpu.SemaphoreType.DMA((8,)),
    )
    names = ('hidden',) + CROSS_IN[2:] + ('wg', 'wu', 'wd') + tuple(name + '_next' for name in WEIGHTS) + ('next_k', 'next_v', 'h2_a', 'h2_b', 'pd_b') + tuple(name + '_out' for name in WEIGHTS) + ('k_a', 'v_a', 'k_b', 'v_b') + tuple(scratch)
    cache = (1,) + self_keys.shape[1:4] + (tc,)
    shapes = [(tc, dim)] * 3 + weight_shapes(dim, heads * head_dim) + [cache] * 4
    return pl.pallas_call(
        functools.partial(block_a_kernel, names),
        in_specs=[HBM_SPEC] * 19,
        out_specs=[VMEM_SPEC] * 11,
        out_shape=[pltpu.VMEM(shape, BF16) for shape in shapes],
        scratch_shapes=list(scratch.values()),
        compiler_params=pltpu.CompilerParams(vmem_limit_bytes=30 << 20, collective_id=0, has_side_effects=True),
        cost_estimate=pl.CostEstimate(flops=20_000_000_000, bytes_accessed=20 << 20, transcendentals=0),
        name="block_a",
    )(hidden, p_a, peer_a, p_b, mask, scale, wq, wo, keys, values, wg, wu, wd, *next_weights, self_keys, self_values)


def block_b_kernel(names, *refs):
    r = t = Refs(names, refs)
    dp, tp, me = lax.axis_index('dp'), lax.axis_index('tp'), lax.axis_index('ep')
    group = lax.axis_size('ep')
    local, cap_rows, dim = t.xin.shape
    capacity = cap_rows // group
    tokens = t.h_scr.shape[0]
    ring = t.wg_ring.shape[0]
    tc = tokens // 2
    half = dim // 2
    lag = 3
    rows_local = local * capacity
    near = (dp, tp, me + 1 - 2 * lax.rem(me, 2))
    across = (dp, tp, lax.rem(me + 2, group))
    others = [(dp, tp, lax.rem(me + k, group)) for k in range(1, group)]
    owners = (me, near[2], across[2], lax.rem(near[2] + 2, group))

    def fetch(i):
        slot = lax.rem(i, ring)
        return [pltpu.make_async_copy(src.at[i], dst.at[slot], t.e_sem.at[n, slot]) for n, (src, dst) in enumerate(((r.wg, t.wg_ring), (r.wu, t.wu_ring), (r.wd, t.wd_ring)))]

    cross = Cross(1, r, t, 3, ('p_b', 'p_a', 'peer_a', 'h_a', 'h_b'))
    cross.start_loads()
    side = [pltpu.make_async_copy(r.router, t.router_scr, t.s_sem.at[0]), pltpu.make_async_copy(r.idx, t.idx_scr, t.s_sem.at[1])]
    for copy in side:
        copy.start()
    greet([tp_peer()] + others)
    early = []
    for i in range(ring):
        early += fetch(i)

    h_a, h_b = cross.run(early)
    t.h_scr[0:tc, :] = h_a
    t.h_scr[tc:, :] = h_b
    def spread(c):
        rows = pl.ds(c * tc, tc)
        mine = t.x_scr.at[0, rows, :]
        return [
            remote(mine, t.x_scr.at[2, rows, :], (t.xs_sem.at[c, 0], t.xr_sem.at[c, 0]), across),
            remote(mine, t.x_scr.at[1, rows, :], (t.xs_sem.at[c, 1], t.xr_sem.at[c, 1]), near),
            remote(t.x_scr.at[2, rows, :], t.x_scr.at[3, rows, :], (t.xs_sem.at[c, 2], t.xr_sem.at[c, 2]), near),
        ]

    def span(owner, i):
        return pl.ds(pl.multiple_of((owner * local + i) * capacity, capacity), capacity)

    def mine(owner):
        return pl.ds(pl.multiple_of(owner * capacity, capacity), capacity)

    def send_back(i, k):
        dst = lax.rem(me + k, group)
        return remote(t.ysum.at[i, mine(dst), :], t.ret.at[span(me, i), :], (t.bs_sem.at[k - 1, i], t.br_sem.at[k - 1, i]), (dp, tp, dst))

    def fold(i):
        return remote(t.yout.at[i], t.yin.at[i], (t.os_sem.at[i], t.or_sem.at[i]), tp_peer())

    def give_back(i):
        fold(i).wait_recv()
        t.ysum[i] = (t.ysum[i].astype(F32) + t.yin[i].astype(F32)).astype(BF16)
        for k in range(1, group):
            send_back(i, k).start()
        t.ret[span(me, i), :] = t.ysum[i, mine(me), :]

    def finish(c):
        rows = slice(c * tc, (c + 1) * tc)
        cross.swaps[1 + c].wait_recv()
        h_cur = add_parts(t.h_scr[rows, :], t.sbuf[c], t.rbuf[1 + c])
        t.h_scr[rows, :] = h_cur
        t.x_scr[0, rows, :] = rms_norm(h_cur, t.scale_scr[2, 1:2, :])
        hops = spread(c)
        hops[0].start()
        hops[1].start()
        return hops

    first = finish(0)
    side[1].wait()
    lane_idx = jnp.broadcast_to(t.idx_scr[...].astype(F32), (tokens, tokens))
    row_idx = jnp.transpose(lane_idx)
    same = lane_idx == row_idx
    row_no = lax.broadcasted_iota(jnp.int32, same.shape, 0)
    lane_no = lax.broadcasted_iota(jnp.int32, same.shape, 1)
    lane_slot = jnp.sum(jnp.where(same & (row_no < lane_no), 1.0, 0.0), axis=0, keepdims=True)
    row_slot = jnp.sum(jnp.where(same & (lane_no < row_no), 1.0, 0.0), axis=1, keepdims=True)
    total = group * rows_local
    lane_dest = jnp.where(lane_slot < capacity, lane_idx[0:1, :] * capacity + lane_slot, -1.0)
    row_dest = jnp.where(row_slot < capacity, row_idx[:, 0:1] * capacity + row_slot, -1.0)
    t.dest[0] = jnp.broadcast_to(lane_dest, t.dest.shape[1:])
    dest_sends = [remote(t.dest.at[0], t.dest.at[k], (t.is_sem.at[k - 1], t.ir_sem.at[k - 1]), (dp, tp, owners[k])) for k in range(1, group)]
    for copy in dest_sends:
        copy.start()
    t.place[...] = (lax.broadcasted_iota(jnp.int32, (tokens, total), 1).astype(F32) == row_dest).astype(BF16)
    t.hot[...] = jnp.where(lax.broadcasted_iota(jnp.int32, t.hot.shape, 1).astype(F32) == row_idx[:, 0:1], 1.0, 0.0)

    second = finish(1)
    first[0].wait_recv()
    first[2].start()
    first_row = (me * rows_local).astype(F32)
    for k in range(group):
        if k:
            dest_sends[k - 1].wait_recv()
        wanted = lax.broadcasted_iota(jnp.int32, (rows_local, tokens), 0).astype(F32) + first_row
        t.pick[k] = (wanted == t.dest[k, 0:1, :]).astype(BF16)
    side[0].wait()
    logits = jnp.dot(t.x_scr[0].astype(F32), t.router_scr[...].T, precision=lax.Precision.HIGHEST, preferred_element_type=F32)
    top = jnp.max(logits, axis=-1, keepdims=True)
    weight = jnp.exp(logits - top)
    weight = weight / jnp.sum(weight, axis=-1, keepdims=True)
    t.gate[...] = jnp.broadcast_to(jnp.sum(t.hot[...] * weight, axis=-1, keepdims=True), t.gate.shape)
    second[0].wait_recv()
    second[2].start()
    for copy in first[1:] + second[1:]:
        copy.wait_recv()
    for k in range(group):
        block = project(t.pick[k], t.x_scr[k]).astype(BF16)
        for i in range(local):
            t.xin[i, mine(owners[k]), :] = block[i * capacity:(i + 1) * capacity, :]

    @pl.loop(0, local)
    def _(i):
        slot = lax.rem(i, ring)
        copies = fetch(i)
        x = t.xin[i]
        for copy in copies:
            copy.wait()
        total_out = None
        for f in range(0, t.wg_ring.shape[2], 768):
            cols = slice(f, f + 768)
            gate_in = jax.nn.gelu(project(x, t.wg_ring[slot, :, cols]))
            product = (gate_in * project(x, t.wu_ring[slot, :, cols])).astype(BF16)
            piece = project(product, t.wd_ring[slot, cols, :])
            total_out = piece if total_out is None else total_out + piece
        result = total_out.astype(BF16)
        @pl.when(i + ring < local)
        def _():
            for copy in fetch(i + ring):
                copy.start()

        low, high = result[:, :half], result[:, half:]
        t.ysum[i] = jnp.where(tp == 0, low, high)
        t.yout[i] = jnp.where(tp == 0, high, low)
        fold(i).start()

        @pl.when(i >= lag)
        def _():
            give_back(i - lag)

    @pl.loop(local - lag, local)
    def _(i):
        give_back(i)

    @pl.loop(0, local)
    def _(i):
        for k in range(1, group):
            send_back(i, k).wait_recv()

    pieces = t.comb.shape[0]
    size = tokens // pieces
    last = [remote(t.comb.at[p], t.comb_peer.at[p], (t.fs_sem.at[p], t.fr_sem.at[p]), tp_peer()) for p in range(pieces)]
    for p in range(pieces):
        t.comb[p] = project(t.place[p * size:(p + 1) * size, :], t.ret[...]).astype(BF16)
        last[p].start()
    for p in range(pieces):
        rows = slice(p * size, (p + 1) * size)
        last[p].wait_recv()
        own, peer = t.comb[p].astype(F32), t.comb_peer[p].astype(F32)
        gate = t.gate[rows, 0:1]
        for side_no, both in enumerate((jnp.where(tp == 0, own, peer), jnp.where(tp == 0, peer, own))):
            cols = slice(side_no * half, (side_no + 1) * half)
            r.out[rows, cols] = (t.h_scr[rows, cols].astype(F32) + gate * both).astype(BF16)
    for copy in cross.swaps + last + dest_sends + first + second:
        copy.wait_send()

    @pl.loop(0, local)
    def _(i):
        fold(i).wait_send()
        for k in range(1, group):
            send_back(i, k).wait_send()


def block_b_call(h_a, h_b, p_a, peer_a, p_b, mask, scale, wq, wo, keys, values, router, idx, wg, wu, wd, group):
    _, heads, slots, head_dim, tokens = keys.shape
    local, dim, ff = wg.shape
    experts = router.shape[0]
    capacity = (2 * tokens + experts - 1) // experts
    ring = 5
    pieces = 4
    scratch = cross_scratch(heads, slots, head_dim, tokens, dim, True, 5)
    hops = (group - 1, local)
    scratch.update(
        wg_ring=pltpu.VMEM((ring, dim, ff), BF16),
        wu_ring=pltpu.VMEM((ring, dim, ff), BF16),
        wd_ring=pltpu.VMEM((ring, ff, dim), BF16),
        router_scr=pltpu.VMEM(router.shape, F32),
        idx_scr=pltpu.VMEM((1, tokens), jnp.int32),
        h_scr=pltpu.VMEM((tokens, dim), BF16),
        x_scr=pltpu.VMEM((group, tokens, dim), BF16),
        dest=pltpu.VMEM((group, 8, tokens), F32),
        hot=pltpu.VMEM((tokens, experts), F32),
        pick=pltpu.VMEM((group, local * capacity, tokens), BF16),
        place=pltpu.VMEM((tokens, experts * capacity), BF16),
        gate=pltpu.VMEM((tokens, 128), F32),
        xin=pltpu.VMEM((local, group * capacity, dim), BF16),
        yout=pltpu.VMEM((local, group * capacity, dim // 2), BF16),
        yin=pltpu.VMEM((local, group * capacity, dim // 2), BF16),
        ysum=pltpu.VMEM((local, group * capacity, dim // 2), BF16),
        ret=pltpu.VMEM((experts * capacity, dim // 2), BF16),
        comb=pltpu.VMEM((pieces, tokens // pieces, dim // 2), BF16),
        comb_peer=pltpu.VMEM((pieces, tokens // pieces, dim // 2), BF16),
        e_sem=pltpu.SemaphoreType.DMA((3, ring)),
        s_sem=pltpu.SemaphoreType.DMA((2,)),
        is_sem=pltpu.SemaphoreType.DMA((group - 1,)),
        ir_sem=pltpu.SemaphoreType.DMA((group - 1,)),
        xs_sem=pltpu.SemaphoreType.DMA((2, 3)),
        xr_sem=pltpu.SemaphoreType.DMA((2, 3)),
        bs_sem=pltpu.SemaphoreType.DMA(hops),
        br_sem=pltpu.SemaphoreType.DMA(hops),
        os_sem=pltpu.SemaphoreType.DMA((local,)),
        or_sem=pltpu.SemaphoreType.DMA((local,)),
        fs_sem=pltpu.SemaphoreType.DMA((pieces,)),
        fr_sem=pltpu.SemaphoreType.DMA((pieces,)),
    )
    names = CROSS_IN + ('router', 'idx', 'wg', 'wu', 'wd', 'out') + tuple(scratch)
    return pl.pallas_call(
        functools.partial(block_b_kernel, names),
        in_specs=[HBM_SPEC] * 16,
        out_specs=VMEM_SPEC,
        out_shape=jax.ShapeDtypeStruct((tokens, dim), BF16),
        scratch_shapes=list(scratch.values()),
        compiler_params=pltpu.CompilerParams(vmem_limit_bytes=B_LIMIT, collective_id=1, has_side_effects=True),
        cost_estimate=pl.CostEstimate(flops=40_000_000_000, bytes_accessed=70 << 20, transcendentals=0),
        name="block_b",
    )(h_a, h_b, p_a, peer_a, p_b, mask, scale, wq, wo, keys, values, router, idx, wg, wu, wd)


def swap(part):
    return part, lax.ppermute(part, 'tp', SWAP)


def decode_body(hidden, write_pos, enc_mask, expert_idx, self_keys, self_values, cross_keys, cross_values, rel_bias, norm_scale, w_query, w_key, w_value, w_out, w_cross_query, w_cross_out, dense_gate, dense_up, dense_down, router, exp_gate, exp_up, exp_down):
    order = (0, 2, 3, 4, 1)
    keys, values = jnp.transpose(self_keys, order), jnp.transpose(self_values, order)
    ckeys, cvalues = jnp.transpose(cross_keys, order), jnp.transpose(cross_values, order)
    pos = write_pos.reshape(1, -1)
    mask = enc_mask.T
    scale = jnp.transpose(norm_scale, (1, 0, 2))
    def hbm(*arrays):
        return [pltpu.with_memory_space_constraint(array, pltpu.HBM) for array in arrays]

    hidden, pos, scale, rel_bias, mask = hbm(hidden, pos, scale, rel_bias, mask)
    w_query, w_key, w_value, w_out, w_cross_query, w_cross_out = hbm(w_query, w_key, w_value, w_out, w_cross_query, w_cross_out)
    keys, values, ckeys, cvalues = hbm(keys, values, ckeys, cvalues)
    dense_gate, dense_up, dense_down, exp_gate, exp_up, exp_down = hbm(dense_gate, dense_up, dense_down, exp_gate, exp_up, exp_down)
    router_t, idx = hbm(router.T, expert_idx.reshape(1, -1))
    shared = (pos, scale, rel_bias, keys, values)
    weights = (w_query, w_key, w_value, w_out)
    cross = (mask, scale, w_cross_query, w_cross_out, ckeys, cvalues)
    p_a, *rest = self_call(0, 0, hidden, *shared, weights=weights)
    held, outs = rest[:4], rest[4:]
    pair_a = swap(p_a)
    p_b, *outs = self_call(0, 1, hidden, *shared, outs=outs, held=held)
    h_a, h_b, pd_b, *rest = block_a_call(hidden, *pair_a, p_b, *cross, dense_gate, dense_up, dense_down, weights, keys, values)
    held, ready_a, ready_b = rest[:4], rest[4:6], rest[6:]
    pair_b = swap(pd_b)
    p_a, *outs = self_call(1, 0, h_a, *shared, outs=outs, held=held, ready=ready_a)
    pair_a = swap(p_a)
    h_b, p_b, *outs = self_call(1, 1, h_b, *shared, outs=outs, parts=pair_b, held=held, ready=ready_b)
    h_all = block_b_call(h_a, h_b, *pair_a, p_b, *cross, router_t, idx, exp_gate, exp_up, exp_down, lax.axis_size('ep'))
    back = (0, 4, 1, 2, 3)
    return h_all, jnp.transpose(outs[0], back), jnp.transpose(outs[1], back)


def solution(mesh):
    batch = ('dp', 'ep')
    row_spec = P(batch, None)
    vec_spec = P(batch)
    cache_spec = P(None, batch, 'tp', None, None)
    col_spec = P(None, None, 'tp')
    out_rows = P(None, 'tp', None)
    in_specs = (row_spec, vec_spec, row_spec, vec_spec, cache_spec, cache_spec, cache_spec, cache_spec, P('tp', None), P(), col_spec, col_spec, col_spec, out_rows, col_spec, out_rows, P(None, 'tp'), P(None, 'tp'), P('tp', None), P(), P('ep', None, 'tp'), P('ep', None, 'tp'), P('ep', 'tp', None))
    out_specs = (row_spec, cache_spec, cache_spec)
    return jax.shard_map(decode_body, mesh=mesh, in_specs=in_specs, out_specs=out_specs, check_vma=False)
```
